32 devices in a mesh: dp: 4 (over y, z), tp: 8 (over x, core).
Axes of the slice: x: 4, y: 2, z: 2, core: 2. Of those that a mesh axis runs over, the one named last changes fastest.
The devices are a block of a 4x4x8 slice.
Arguments:
- x: bfloat16 [32, 576, 1024], P('dp', 'tp'), parts along dimension 0
- d_out: bfloat16 [32, 576, 1024], P('dp', 'tp'), parts along dimension 0
- ln1_gain: float32 [1024], replicated
- ln1_bias: float32 [1024], replicated
- w_q: bfloat16 [1024, 16, 64], P(None, 'tp')
- b_q: bfloat16 [16, 64], P('tp')
- w_k: bfloat16 [1024, 16, 64], P(None, 'tp')
- w_v: bfloat16 [1024, 16, 64], P(None, 'tp')
- b_v: bfloat16 [16, 64], P('tp')
- w_o: bfloat16 [16, 64, 1024], P('tp')
- b_o: bfloat16 [1024], replicated
- ln2_gain: float32 [1024], replicated
- ln2_bias: float32 [1024], replicated
- w_1: bfloat16 [1024, 4096], P(None, 'tp')
- b_1: bfloat16 [4096], P('tp')
- w_2: bfloat16 [4096, 1024], P('tp')
- b_2: bfloat16 [1024], replicated
Outputs:
- output 1: bfloat16 [32, 576, 1024], P('dp', 'tp'), parts along dimension 0
- output 2: bfloat16 [32, 576, 1024], P('dp', 'tp'), parts along dimension 0
- output 3: float32 [4096], P('dp'), parts along dimension 0
- output 4: float32 [4096], P('dp'), parts along dimension 0
- output 5: bfloat16 [4096, 16, 64], P('dp', 'tp'), parts along dimension 0
- output 6: bfloat16 [64, 64], P(('dp', 'tp')), parts along dimension 0
- output 7: bfloat16 [4096, 16, 64], P('dp', 'tp'), parts along dimension 0
- output 8: bfloat16 [4096, 16, 64], P('dp', 'tp'), parts along dimension 0
- output 9: bfloat16 [64, 64], P(('dp', 'tp')), parts along dimension 0
- output 10: bfloat16 [64, 64, 1024], P(('dp', 'tp')), parts along dimension 0
- output 11: bfloat16 [4096], P('dp'), parts along dimension 0
- output 12: float32 [4096], P('dp'), parts along dimension 0
- output 13: float32 [4096], P('dp'), parts along dimension 0
- output 14: bfloat16 [4096, 4096], P('dp', 'tp'), parts along dimension 0
- output 15: bfloat16 [16384], P(('dp', 'tp')), parts along dimension 0
- output 16: bfloat16 [16384, 1024], P(('dp', 'tp')), parts along dimension 0
- output 17: bfloat16 [4096], P('dp'), parts along dimension 0
There are 4 independent parts. The reference program is written for one: setup_inputs(seed, part) draws one part's arguments, and reference() takes and returns one part's arrays. A program takes and returns all parts, laid end to end along the dimension named above; an argument that names none is the same for every part.
All inputs are finite; a program needn't handle non-finite values.
Results may differ from the reference program's by a relative error of at most 0.0187366.
Values are sent between devices in bfloat16 or wider.
A program may use at most 768 MiB of HBM per device.

```python
import math
import jax
import jax.numpy as jnp
from jax import lax

IMAGES = 8
PATCHES = 576
WIDTH = 1024
NUM_HEADS = 16
HEAD_DIM = 64
MLP_DIM = 4096
LN_EPS = 1e-6
ATT_SCALE = 1.0 / math.sqrt(HEAD_DIM)
TOKENS = IMAGES * PATCHES


def draw_normal(key, shape, scale):
    return jax.random.normal(key, shape, jnp.float32) * scale


def setup_inputs(seed: int = 0, part: int = 0) -> dict:
    part_key = jax.random.fold_in(jax.random.key(seed), part)
    act_keys = jax.random.split(part_key, 4)
    wt_keys = jax.random.split(jax.random.key(seed + 1), 15)
    act_shape = (IMAGES, PATCHES, WIDTH)
    row_scale = jnp.exp(draw_normal(act_keys[0], (IMAGES, PATCHES, 1), 0.5))
    row_shift = draw_normal(act_keys[1], (IMAGES, PATCHES, 1), 0.5)
    x = (draw_normal(act_keys[2], act_shape, 1.0) * row_scale + row_shift).astype(jnp.bfloat16)
    d_out = draw_normal(act_keys[3], act_shape, 1.0).astype(jnp.bfloat16)
    in_scale = WIDTH ** -0.5
    qk_scale = in_scale * math.sqrt(math.sqrt(math.log(PATCHES / 8.0)))
    head_w = (WIDTH, NUM_HEADS, HEAD_DIM)
    head_b = (NUM_HEADS, HEAD_DIM)
    return {
        'x': x,
        'd_out': d_out,
        'ln1_gain': 1.0 + draw_normal(wt_keys[0], (WIDTH,), 0.25),
        'ln1_bias': draw_normal(wt_keys[1], (WIDTH,), 0.3),
        'w_q': draw_normal(wt_keys[2], head_w, qk_scale).astype(jnp.bfloat16),
        'b_q': draw_normal(wt_keys[3], head_b, 0.5).astype(jnp.bfloat16),
        'w_k': draw_normal(wt_keys[4], head_w, qk_scale).astype(jnp.bfloat16),
        'w_v': draw_normal(wt_keys[5], head_w, in_scale).astype(jnp.bfloat16),
        'b_v': draw_normal(wt_keys[6], head_b, 0.5).astype(jnp.bfloat16),
        'w_o': draw_normal(wt_keys[7], (NUM_HEADS, HEAD_DIM, WIDTH), 2.5 * in_scale).astype(jnp.bfloat16),
        'b_o': draw_normal(wt_keys[8], (WIDTH,), 0.5).astype(jnp.bfloat16),
        'ln2_gain': 1.0 + draw_normal(wt_keys[9], (WIDTH,), 0.25),
        'ln2_bias': draw_normal(wt_keys[10], (WIDTH,), 0.3),
        'w_1': draw_normal(wt_keys[11], (WIDTH, MLP_DIM), in_scale).astype(jnp.bfloat16),
        'b_1': draw_normal(wt_keys[12], (MLP_DIM,), 0.5).astype(jnp.bfloat16),
        'w_2': draw_normal(wt_keys[13], (MLP_DIM, WIDTH), 1.5 * MLP_DIM ** -0.5).astype(jnp.bfloat16),
        'b_2': draw_normal(wt_keys[14], (WIDTH,), 0.5).astype(jnp.bfloat16),
    }


def layer_norm(rows, ln_gain, ln_bias):
    row_mean = jnp.mean(rows, axis=-1, keepdims=True)
    centered = rows - row_mean
    variance = jnp.mean(centered * centered, axis=-1, keepdims=True)
    return centered * lax.rsqrt(variance + LN_EPS) * ln_gain + ln_bias


def attend_image(qkv_image):
    queries, keys, values = qkv_image
    scores = jnp.einsum('qhd,khd->hqk', queries.astype(jnp.float32), keys.astype(jnp.float32)) * ATT_SCALE
    probs = jax.nn.softmax(scores, axis=-1).astype(jnp.bfloat16)
    mixed = jnp.einsum('hqk,khd->qhd', probs.astype(jnp.float32), values.astype(jnp.float32))
    return mixed.astype(jnp.bfloat16)


def forward(x, ln1_gain, ln1_bias, w_q, b_q, w_k, w_v, b_v, w_o, b_o, ln2_gain, ln2_bias, w_1, b_1, w_2, b_2):
    x_f32 = x.reshape(TOKENS, WIDTH).astype(jnp.float32)
    h_one = layer_norm(x_f32, ln1_gain, ln1_bias).astype(jnp.bfloat16)
    w_qkv = jnp.concatenate([w_q.reshape(WIDTH, WIDTH), w_k.reshape(WIDTH, WIDTH), w_v.reshape(WIDTH, WIDTH)], axis=1)
    b_qkv = jnp.concatenate([b_q.reshape(WIDTH).astype(jnp.float32), jnp.zeros((WIDTH,), jnp.float32), b_v.reshape(WIDTH).astype(jnp.float32)])
    qkv = (jnp.dot(h_one, w_qkv, preferred_element_type=jnp.float32) + b_qkv).astype(jnp.bfloat16)
    head_shape = (IMAGES, PATCHES, NUM_HEADS, HEAD_DIM)
    queries = qkv[:, :WIDTH].reshape(head_shape)
    keys = qkv[:, WIDTH:2 * WIDTH].reshape(head_shape)
    values = qkv[:, 2 * WIDTH:].reshape(head_shape)
    mixed = lax.map(attend_image, (queries, keys, values)).reshape(TOKENS, WIDTH)
    attn_out = jnp.dot(mixed, w_o.reshape(WIDTH, WIDTH), preferred_element_type=jnp.float32)
    x_mid = (x_f32 + attn_out + b_o).astype(jnp.bfloat16)
    mid_f32 = x_mid.astype(jnp.float32)
    h_two = layer_norm(mid_f32, ln2_gain, ln2_bias).astype(jnp.bfloat16)
    pre_act = (jnp.dot(h_two, w_1, preferred_element_type=jnp.float32) + b_1).astype(jnp.bfloat16)
    hidden = jax.nn.gelu(pre_act.astype(jnp.float32), approximate=True).astype(jnp.bfloat16)
    mlp_out = jnp.dot(hidden, w_2, preferred_element_type=jnp.float32)
    y_out = (mid_f32 + mlp_out + b_2).astype(jnp.bfloat16)
    return y_out.reshape(IMAGES, PATCHES, WIDTH)


def reference(x, d_out, ln1_gain, ln1_bias, w_q, b_q, w_k, w_v, b_v, w_o, b_o, ln2_gain, ln2_bias, w_1, b_1, w_2, b_2):
    y_out, pullback = jax.vjp(forward, x, ln1_gain, ln1_bias, w_q, b_q, w_k, w_v, b_v, w_o, b_o, ln2_gain, ln2_bias, w_1, b_1, w_2, b_2)
    (grad_x, grad_ln1_gain, grad_ln1_bias, grad_w_q, grad_b_q, grad_w_k, grad_w_v, grad_b_v, grad_w_o, grad_b_o,
     grad_ln2_gain, grad_ln2_bias, grad_w_1, grad_b_1, grad_w_2, grad_b_2) = pullback(d_out)
    return (y_out, grad_x, grad_ln1_gain, grad_ln1_bias, grad_w_q, grad_b_q, grad_w_k, grad_w_v, grad_b_v, grad_w_o, grad_b_o,
            grad_ln2_gain, grad_ln2_bias, grad_w_1, grad_b_1, grad_w_2, grad_b_2)
```

```python
import math
import jax
import jax.numpy as jnp
from jax import lax
from jax.sharding import PartitionSpec as P

LN_EPS = 1e-6
F32 = jnp.float32
BF16 = jnp.bfloat16


def layer_norm(rows, ln_gain, ln_bias):
    row_mean = jnp.mean(rows, axis=-1, keepdims=True)
    centered = rows - row_mean
    variance = jnp.mean(centered * centered, axis=-1, keepdims=True)
    return centered * lax.rsqrt(variance + LN_EPS) * ln_gain + ln_bias


def gelu_tanh(pre_act):
    return jax.nn.gelu(pre_act, approximate=True)


def dot(eq, a, b):
    return jnp.einsum(eq, a, b, preferred_element_type=F32)


def attention_core(qkv):
    g, n, f = qkv.shape
    hd = 64
    h = f // (3 * hd)
    parts = qkv.reshape(g, n, 3, h, hd)
    queries, keys, values = parts[:, :, 0], parts[:, :, 1], parts[:, :, 2]
    att_scale = 1.0 / math.sqrt(hd)
    scores = dot('gqhd,gkhd->ghqk', queries, keys) * att_scale
    probs = jax.nn.softmax(scores, axis=-1).astype(BF16)
    mixed = dot('ghqk,gkhd->gqhd', probs, values)
    return mixed.astype(BF16).reshape(g, n, h * hd)


def solution(mesh):
    act_spec = P('dp', 'tp', None)
    replicated = P()
    head_w = P(None, 'tp', None)
    head_b = P('tp', None)
    grad_head_w = P('dp', 'tp', None)
    grad_head_b = P(('dp', 'tp'), None)
    grad_vec = P('dp')
    in_specs = (act_spec, act_spec, replicated, replicated, head_w, head_b, head_w, head_w, head_b,
                P('tp', None, None), replicated, replicated, replicated, P(None, 'tp'), P('tp'), P('tp', None), replicated)
    out_specs = (act_spec, act_spec, grad_vec, grad_vec, grad_head_w, grad_head_b, grad_head_w, grad_head_w, grad_head_b,
                 P(('dp', 'tp'), None, None), grad_vec, grad_vec, grad_vec, P('dp', 'tp'), P(('dp', 'tp')),
                 P(('dp', 'tp'), None), grad_vec)

    def gather(a):
        return lax.all_gather(a, 'tp', axis=0, tiled=False)

    def to_image(a):
        return lax.all_to_all(a, 'tp', split_axis=0, concat_axis=1, tiled=True)

    def to_tokens(a):
        return lax.all_to_all(a, 'tp', split_axis=1, concat_axis=0, tiled=True)

    def layer_step(x, d_out, ln1_gain, ln1_bias, w_q, b_q, w_k, w_v, b_v, w_o, b_o, ln2_gain, ln2_bias, w_1, b_1, w_2, b_2):
        width = x.shape[-1]
        heads_loc, hd = w_q.shape[1:]
        hw = heads_loc * hd
        wqkv_loc = jnp.concatenate([w.reshape(width, hw) for w in (w_q, w_k, w_v)], axis=1)
        bqkv_loc = jnp.concatenate([b_q.reshape(hw), jnp.zeros((hw,), b_q.dtype), b_v.reshape(hw)])
        wqkv = gather(wqkv_loc)
        bqkv = gather(bqkv_loc)
        wo = gather(w_o.reshape(hw, width))
        w1 = gather(w_1)
        b1 = gather(b_1)
        w2 = gather(w_2)
        d_out_all = lax.all_gather(d_out, 'tp', axis=1, tiled=True)
        me = lax.axis_index('tp')

        xi = to_image(x)[0]
        x_f32 = xi.astype(F32)
        h_one_f, ln1_pull = jax.vjp(layer_norm, x_f32, ln1_gain, ln1_bias)
        h_one = h_one_f.astype(BF16)
        qkv = (dot('nw,dwf->dnf', h_one, wqkv) + bqkv[:, None, :]).astype(BF16)
        mixed, attn_pull = jax.vjp(attention_core, qkv)
        attn_out = dot('dnf,dfw->nw', mixed, wo)
        x_mid = (x_f32 + attn_out + b_o).astype(BF16)
        mid_f32 = x_mid.astype(F32)
        h_two_f, ln2_pull = jax.vjp(layer_norm, mid_f32, ln2_gain, ln2_bias)
        h_two = h_two_f.astype(BF16)
        h_two_all = gather(h_two)
        pre_act = (dot('nw,dwf->dnf', h_two, w1) + b1[:, None, :]).astype(BF16)
        hidden_f, gelu_pull = jax.vjp(gelu_tanh, pre_act.astype(F32))
        hidden = hidden_f.astype(BF16)
        mlp_out = dot('dnf,dfw->nw', hidden, w2)
        y_img = (mid_f32 + mlp_out + b_2).astype(BF16)
        y_out = to_tokens(y_img[None])

        d_img = lax.dynamic_index_in_dim(d_out_all, me, 0, keepdims=False)
        d_hidden = dot('nw,dfw->dnf', d_img, w2).astype(BF16)
        (d_pre_f,) = gelu_pull(d_hidden.astype(F32))
        d_pre = d_pre_f.astype(BF16)
        d_h_two = dot('dnf,dwf->nw', d_pre, w1).astype(BF16)
        d_mid_ln, g_ln2_gain, g_ln2_bias = ln2_pull(d_h_two.astype(F32))
        d_mid = (d_img.astype(F32) + d_mid_ln).astype(BF16)
        d_mixed = dot('nw,dfw->dnf', d_mid, wo).astype(BF16)
        g_wo_part = dot('dnf,nw->dfw', mixed, d_mid)
        grad_w_o = lax.psum_scatter(g_wo_part, 'tp', scatter_dimension=0).astype(BF16).reshape(w_o.shape)
        (d_qkv,) = attn_pull(d_mixed)
        g_qkv_part = dot('nw,dnf->dwf', h_one, d_qkv)
        g_qkv = lax.psum_scatter(g_qkv_part, 'tp', scatter_dimension=0).astype(BF16)
        d_h_one = dot('dnf,dwf->nw', d_qkv, wqkv).astype(BF16)
        d_in_ln, g_ln1_gain, g_ln1_bias = ln1_pull(d_h_one.astype(F32))
        gx_img = (d_mid.astype(F32) + d_in_ln).astype(BF16)
        grad_x = to_tokens(gx_img[None])

        u_loc = (dot('bnw,wf->bnf', h_two_all, w_1) + b_1).astype(BF16)
        g_loc_f, gelu_pull2 = jax.vjp(gelu_tanh, u_loc.astype(F32))
        g_loc = g_loc_f.astype(BF16)
        dh_loc = dot('bnw,fw->bnf', d_out_all, w_2).astype(BF16)
        (dp_f,) = gelu_pull2(dh_loc.astype(F32))
        dp = dp_f.astype(BF16)
        grad_b_1 = jnp.sum(dp, axis=(0, 1), dtype=F32).astype(BF16)
        grad_w_1 = dot('bnw,bnf->wf', h_two_all, dp).astype(BF16)
        grad_w_2 = dot('bnf,bnw->fw', g_loc, d_out_all).astype(BF16)

        g_b_part = jnp.sum(d_qkv, axis=1, dtype=F32).reshape(-1, width)
        vec = jnp.concatenate([jnp.stack([g_ln1_gain, g_ln1_bias, g_ln2_gain, g_ln2_bias,
                                          jnp.sum(d_mid, axis=0, dtype=F32), jnp.sum(d_img, axis=0, dtype=F32)]), g_b_part])
        vec = lax.psum(vec, 'tp')
        gb = lax.dynamic_index_in_dim(vec[6:].reshape(-1, 3 * hw), me, 0, keepdims=False)
        grad_b_q = gb[:hw].astype(BF16).reshape(b_q.shape)
        grad_b_v = gb[2 * hw:].astype(BF16).reshape(b_v.shape)
        gq, gk, gv = (g_qkv[:, i * hw:(i + 1) * hw].reshape(w_q.shape) for i in range(3))
        return (y_out, grad_x, vec[0], vec[1], gq, grad_b_q, gk, gv, grad_b_v, grad_w_o,
                vec[4].astype(BF16), vec[2], vec[3], grad_w_1, grad_b_1, grad_w_2, vec[5].astype(BF16))

    return jax.shard_map(layer_step, mesh=mesh, in_specs=in_specs, out_specs=out_specs, check_vma=False)
```

```python
import functools
import math
import jax
import jax.numpy as jnp
from jax import lax
from jax.experimental import pallas as pl
from jax.experimental.pallas import tpu as pltpu
from jax.sharding import PartitionSpec as P

LN_EPS = 1e-6
F32 = jnp.float32
BF16 = jnp.bfloat16
NN = (((1,), (0,)), ((), ()))
NT = (((1,), (1,)), ((), ()))
TN = (((0,), (0,)), ((), ()))


def mm(a, b, dims):
    return lax.dot_general(a, b, dims, preferred_element_type=F32)


def layer_norm(rows, ln_gain, ln_bias):
    row_mean = jnp.mean(rows, axis=-1, keepdims=True)
    centered = rows - row_mean
    variance = jnp.mean(centered * centered, axis=-1, keepdims=True)
    return centered * lax.rsqrt(variance + LN_EPS) * ln_gain + ln_bias


def gelu_tanh(pre_act):
    return jax.nn.gelu(pre_act, approximate=True)


def dot(eq, a, b):
    return jnp.einsum(eq, a, b, preferred_element_type=F32)


def attn_fwd_kernel(heads, hd, h_ref, w_ref, b_ref, qkv_ref, mix_ref, st_ref, acc_ref):
    hw = heads * hd
    scale = 1.0 / math.sqrt(hd)
    qkv = (mm(w_ref[0, :3 * hw], h_ref[...], NT) + b_ref[0]).astype(BF16)
    qkv_ref[0] = qkv
    for h in range(heads):
        q = qkv[h * hd:(h + 1) * hd]
        k = qkv[hw + h * hd:hw + (h + 1) * hd]
        v = qkv[2 * hw + h * hd:2 * hw + (h + 1) * hd]
        s = mm(k, q, TN) * scale
        top = jnp.max(s, axis=0, keepdims=True)
        e = jnp.exp(s - top)
        inv = 1.0 / jnp.sum(e, axis=0, keepdims=True)
        st_ref[0, 2 * h:2 * h + 1] = top
        st_ref[0, 2 * h + 1:2 * h + 2] = inv
        p = (e * inv).astype(BF16)
        mix_ref[0, h * hd:(h + 1) * hd] = mm(v, p, NN).astype(BF16)
    part = mm(mix_ref[0], w_ref[0, 3 * hw:4 * hw], TN)

    @pl.when(pl.program_id(0) == 0)
    def _():
        acc_ref[...] = part

    @pl.when(pl.program_id(0) > 0)
    def _():
        acc_ref[...] += part


def attn_fwd(h_one, wcat, bias_col, heads, hd):
    g, rows, width = wcat.shape
    n = h_one.shape[0]
    hw = heads * hd
    full = lambda shape: pl.BlockSpec(shape, lambda i: (0,) * len(shape))
    blk = lambda shape: pl.BlockSpec((1,) + shape, lambda i: (i,) + (0,) * len(shape))
    return pl.pallas_call(
        functools.partial(attn_fwd_kernel, heads, hd),
        grid=(g,),
        in_specs=[full((n, width)), blk((rows, width)), blk((3 * hw, 1))],
        out_specs=[blk((3 * hw, n)), blk((hw, n)), blk((2 * heads, n)), full((n, width))],
        out_shape=[jax.ShapeDtypeStruct((g, 3 * hw, n), BF16), jax.ShapeDtypeStruct((g, hw, n), BF16),
                   jax.ShapeDtypeStruct((g, 2 * heads, n), F32), jax.ShapeDtypeStruct((n, width), F32)],
        compiler_params=pltpu.CompilerParams(dimension_semantics=("arbitrary",), vmem_limit_bytes=60 << 20),
        cost_estimate=pl.CostEstimate(flops=20_000_000_000, bytes_accessed=20_000_000, transcendentals=0),
        name="attn_fwd",
    )(h_one, wcat, bias_col)


def gelu_and_slope(u):
    c = math.sqrt(2.0 / math.pi)
    u2 = u * u
    t = jnp.tanh(c * (u + 0.044715 * (u2 * u)))
    half = 0.5 * (1.0 + t)
    slope = half + 0.5 * u * (1.0 - t * t) * (c * (1.0 + (3.0 * 0.044715) * u2))
    return u * half, slope


def block_of_step(j, size):
    me = lax.axis_index('tp')
    chips = size // 2
    off = jnp.where(j < 2, 2, jnp.where(j < 4, 1, jnp.where(j < 6, 3, 0)))
    chip = lax.rem(lax.div(me, 2) + off, chips)
    core = lax.rem(me, 2)
    side = jnp.where(lax.rem(j, 2) == 0, 1 - core, core)
    return 2 * chip + side


def layer_bwd_kernel(heads, hd, size, h_ref, dm_ref, w_ref, qkv_ref, mix_ref, st_ref, h2_ref, do_ref, w1_ref, w2_ref, b1_ref,
                     g_ref, db_ref, dh_ref, gw1_ref, gw2_ref, gb1_ref,
                     dqkv_ref, pair_out, own, pair_in, opp_l, opp_r, near_l, near_r, acc1, acc2,
                     pair_send, pair_recv, opp_send, opp_recv, near_send, near_recv):
    hw = heads * hd
    scale = 1.0 / math.sqrt(hd)
    j = pl.program_id(0)
    me = lax.axis_index('tp')
    core = lax.rem(me, 2)
    partner = me + 1 - 2 * core
    right = lax.rem(me + 2, size)
    left = lax.rem(me + size - 2, size)
    half = 2 * hw

    def send(src, dst, ssem, rsem, dev):
        return pltpu.make_async_remote_copy(src_ref=src, dst_ref=dst, send_sem=ssem, recv_sem=rsem,
                                            device_id={'tp': dev}, device_id_type=pl.DeviceIdType.MESH)

    def pair_copy(t):
        return send(pair_out.at[t % 2], pair_in.at[t], pair_send.at[t], pair_recv.at[t], partner)

    lo, hi = pl.ds(0, half), pl.ds(half, half)
    opp_right = lambda: send(own.at[0, lo], opp_l, opp_send.at[0], opp_recv.at[0], right)
    opp_left = lambda: send(own.at[0, hi], opp_r, opp_send.at[1], opp_recv.at[1], left)
    right_hi = lambda: send(own.at[1, hi], near_l.at[hi], near_send.at[0], near_recv.at[0], right)
    right_lo = lambda: send(own.at[1, lo], near_l.at[lo], near_send.at[1], near_recv.at[1], right)
    left_lo = lambda: send(own.at[2, lo], near_r.at[lo], near_send.at[2], near_recv.at[2], left)
    left_hi = lambda: send(own.at[2, hi], near_r.at[hi], near_send.at[3], near_recv.at[3], left)

    @pl.when(j == 0)
    def _():
        barrier = pltpu.get_barrier_semaphore()
        for dev in (partner, right, left):
            pl.semaphore_signal(barrier, inc=1, device_id={'tp': dev}, device_id_type=pl.DeviceIdType.MESH)
        pl.semaphore_wait(barrier, 3)

    @pl.when(j < size)
    def _():
        d_mix = mm(w_ref[0, 3 * hw:4 * hw], dm_ref[...], NT).astype(BF16)
        qkv = qkv_ref[0]
        for h in range(heads):
            q = qkv[h * hd:(h + 1) * hd]
            k = qkv[hw + h * hd:hw + (h + 1) * hd]
            v = qkv[2 * hw + h * hd:2 * hw + (h + 1) * hd]
            da = d_mix[h * hd:(h + 1) * hd]
            s = mm(k, q, TN) * scale
            p = jnp.exp(s - st_ref[0, 2 * h:2 * h + 1]) * st_ref[0, 2 * h + 1:2 * h + 2]
            dp = mm(v, da, TN).astype(BF16).astype(F32)
            ds = (p * (dp - jnp.sum(p * dp, axis=0, keepdims=True)) * scale).astype(BF16)
            dqkv_ref[h * hd:(h + 1) * hd] = mm(k, ds, NN).astype(BF16)
            dqkv_ref[hw + h * hd:hw + (h + 1) * hd] = mm(q, ds, NT).astype(BF16)
            dqkv_ref[2 * hw + h * hd:2 * hw + (h + 1) * hd] = mm(da, p.astype(BF16), NT).astype(BF16)
        dqkv = dqkv_ref[...]
        db_ref[0] = jnp.sum(dqkv.astype(F32), axis=1, keepdims=True)
        part = mm(dqkv, w_ref[0, :3 * hw], TN)

        @pl.when(j == 0)
        def _():
            dh_ref[...] = part

        @pl.when(j > 0)
        def _():
            dh_ref[...] += part

        for t in range(2, size // 2):
            @pl.when(j == 2 * t)
            def _():
                pair_copy(t - 2).wait_send()

        def grads(out):
            out[:3 * hw] = mm(dqkv_ref[...], h_ref[...], NN)
            out[3 * hw:] = mm(mix_ref[0], dm_ref[...], NN)

        @pl.when(lax.rem(j, 2) == 0)
        def _():
            grads(pair_out.at[lax.rem(lax.div(j, 2), 2)])

        @pl.when(lax.rem(j, 2) == 1)
        def _():
            grads(own.at[lax.div(j, 2)])

        for t in range(size // 2):
            @pl.when(j == 2 * t)
            def _():
                pair_copy(t).start()

            @pl.when(j == 2 * t + 1)
            def _():
                pair_copy(t).wait_recv()
                own[t] += pair_in[t]

        @pl.when(j == 1)
        def _():
            opp_right().start()
            opp_left().start()

        @pl.when(j == 3)
        def _():
            right_hi().start()

        @pl.when(j == 5)
        def _():
            left_lo().start()

        @pl.when(j == 7)
        def _():
            opp_right().wait_recv()
            own[1, lo] += opp_l[...]
            right_lo().start()
            opp_left().wait_recv()
            own[2, hi] += opp_r[...]
            left_hi().start()

    @pl.when(j >= size)
    def _():
        h2 = h2_ref[0]
        do = do_ref[0]
        u = (mm(w1_ref[...], h2, NT) + b1_ref[...]).astype(BF16).astype(F32)
        dg = mm(w2_ref[...], do, NT).astype(BF16).astype(F32)
        g, slope = gelu_and_slope(u)
        du = (dg * slope).astype(BF16)
        g1 = mm(du, h2, NN)
        g2 = mm(g.astype(BF16), do, NN)
        gb = jnp.sum(du.astype(F32), axis=1, keepdims=True)

        @pl.when(j == size)
        def _():
            acc1[...] = g1
            acc2[...] = g2
            gb1_ref[...] = gb

        @pl.when(j > size)
        def _():
            acc1[...] += g1
            acc2[...] += g2
            gb1_ref[...] += gb

    @pl.when(j == 2 * size - 1)
    def _():
        gw1_ref[...] = acc1[...].astype(BF16)
        gw2_ref[...] = acc2[...].astype(BF16)
        for c in (right_hi(), right_lo(), left_lo(), left_hi()):
            c.wait_recv()
        g_ref[...] = (own[3] + near_l[...] + near_r[...]).astype(BF16)
        for t in (size // 2 - 2, size // 2 - 1):
            pair_copy(t).wait_send()
        for c in (opp_right(), opp_left(), right_hi(), right_lo(), left_lo(), left_hi()):
            c.wait_send()


def layer_bwd(h_one, d_mid, wcat, qkv, mix, stats, h2_all, do_all, w1t, w2, b1_col, heads, hd):
    size, rows, width = wcat.shape
    n = h_one.shape[0]
    mlp = w2.shape[0]
    hw = heads * hd
    full = lambda shape: pl.BlockSpec(shape, lambda i: (0,) * len(shape))
    blk = lambda shape: pl.BlockSpec((1,) + shape, lambda i: (block_of_step(jnp.minimum(i, size - 1), size),) + (0,) * len(shape))
    img = lambda shape: pl.BlockSpec((1,) + shape, lambda i: (jnp.maximum(i - size, 0),) + (0,) * len(shape))
    buf = lambda *shape: pltpu.VMEM(shape, F32)
    dma = lambda k: pltpu.SemaphoreType.DMA((k,))
    return pl.pallas_call(
        functools.partial(layer_bwd_kernel, heads, hd, size),
        grid=(2 * size,),
        in_specs=[full((n, width)), full((n, width)), blk((rows, width)), blk((3 * hw, n)), blk((hw, n)), blk((2 * heads, n)),
                  img((n, width)), img((n, width)), full((mlp, width)), full((mlp, width)), full((mlp, 1))],
        out_specs=[full((4 * hw, width)), blk((3 * hw, 1)), full((n, width)), full((mlp, width)), full((mlp, width)), full((mlp, 1))],
        out_shape=[jax.ShapeDtypeStruct((4 * hw, width), BF16), jax.ShapeDtypeStruct((size, 3 * hw, 1), F32),
                   jax.ShapeDtypeStruct((n, width), F32), jax.ShapeDtypeStruct((mlp, width), BF16),
                   jax.ShapeDtypeStruct((mlp, width), BF16), jax.ShapeDtypeStruct((mlp, 1), F32)],
        scratch_shapes=[pltpu.VMEM((3 * hw, n), BF16), buf(2, 4 * hw, width), buf(size // 2, 4 * hw, width), buf(size // 2, 4 * hw, width),
                        buf(2 * hw, width), buf(2 * hw, width), buf(4 * hw, width), buf(4 * hw, width),
                        buf(mlp, width), buf(mlp, width), dma(size // 2), dma(size // 2), dma(2), dma(2), dma(4), dma(4)],
        compiler_params=pltpu.CompilerParams(dimension_semantics=("arbitrary",), vmem_limit_bytes=67_043_328,
                                             collective_id=2, has_side_effects=True),
        cost_estimate=pl.CostEstimate(flops=80_000_000_000, bytes_accessed=80_000_000, transcendentals=0),
        name="layer_bwd",
    )(h_one, d_mid, wcat, qkv, mix, stats, h2_all, do_all, w1t, w2, b1_col)


def sum_kernel(size, v_ref, o_ref, buf, send_sem, recv_sem):
    me = lax.axis_index('tp')
    barrier = pltpu.get_barrier_semaphore()
    for r in range(1, size):
        pl.semaphore_signal(barrier, inc=1, device_id={'tp': lax.rem(me + r, size)}, device_id_type=pl.DeviceIdType.MESH)
    pl.semaphore_wait(barrier, size - 1)
    copies = []
    for r in range(1, size):
        c = pltpu.make_async_remote_copy(src_ref=v_ref, dst_ref=buf.at[me], send_sem=send_sem.at[r - 1], recv_sem=recv_sem.at[r - 1],
                                         device_id={'tp': lax.rem(me + r, size)}, device_id_type=pl.DeviceIdType.MESH)
        c.start()
        copies.append(c)
    buf[me] = v_ref[...]
    for c in copies:
        c.wait()
    total = buf[0]
    for i in range(1, size):
        total += buf[i]
    o_ref[...] = total


def group_sum(v, size):
    return pl.pallas_call(
        functools.partial(sum_kernel, size),
        out_shape=jax.ShapeDtypeStruct(v.shape, F32),
        in_specs=[pl.BlockSpec(memory_space=pltpu.VMEM)],
        out_specs=pl.BlockSpec(memory_space=pltpu.VMEM),
        scratch_shapes=[pltpu.VMEM((size,) + v.shape, F32), pltpu.SemaphoreType.DMA((size - 1,)), pltpu.SemaphoreType.DMA((size - 1,))],
        compiler_params=pltpu.CompilerParams(collective_id=1, has_side_effects=True),
        name="group_sum",
    )(v)


def solution(mesh):
    act_spec = P('dp', 'tp', None)
    replicated = P()
    head_w = P(None, 'tp', None)
    head_b = P('tp', None)
    grad_head_w = P('dp', 'tp', None)
    grad_head_b = P(('dp', 'tp'), None)
    grad_vec = P('dp')
    in_specs = (act_spec, act_spec, replicated, replicated, head_w, head_b, head_w, head_w, head_b,
                P('tp', None, None), replicated, replicated, replicated, P(None, 'tp'), P('tp'), P('tp', None), replicated)
    out_specs = (act_spec, act_spec, grad_vec, grad_vec, grad_head_w, grad_head_b, grad_head_w, grad_head_w, grad_head_b,
                 P(('dp', 'tp'), None, None), grad_vec, grad_vec, grad_vec, P('dp', 'tp'), P(('dp', 'tp')),
                 P(('dp', 'tp'), None), grad_vec)

    def gather(a):
        return lax.all_gather(a, 'tp', axis=0, tiled=False)

    def to_tokens(a):
        n, w = a.shape
        size = mesh.shape['tp']
        return lax.all_to_all(a.reshape(size, n // size, w), 'tp', split_axis=0, concat_axis=0, tiled=True)

    def layer_step(x, d_out, ln1_gain, ln1_bias, w_q, b_q, w_k, w_v, b_v, w_o, b_o, ln2_gain, ln2_bias, w_1, b_1, w_2, b_2):
        width = x.shape[-1]
        heads_loc, hd = w_q.shape[1:]
        hw = heads_loc * hd
        size = mesh.shape['tp']
        mlp_loc = b_1.shape[0]
        flat = lambda w: w.reshape(width, hw).T
        bias_row = jnp.concatenate([b_q.reshape(hw), jnp.zeros((hw,), BF16), b_v.reshape(hw), b_1])
        bias_rows = jnp.zeros((16, width), BF16).at[0, :bias_row.shape[0]].set(bias_row)
        wcat = gather(jnp.concatenate([flat(w_q), flat(w_k), flat(w_v), w_o.reshape(hw, width), bias_rows]))
        bias_all = wcat[:, 4 * hw].astype(F32)
        bqkv_col = bias_all[:, :3 * hw, None]
        b1 = bias_all[:, 3 * hw:3 * hw + mlp_loc]
        w1 = gather(w_1)
        w2 = gather(w_2)
        d_out_all = lax.all_gather(d_out, 'tp', axis=1, tiled=True)
        me = lax.axis_index('tp')

        xi = lax.all_to_all(x, 'tp', split_axis=0, concat_axis=0, tiled=True).reshape(-1, width)
        x_f32 = xi.astype(F32)
        h_one_f, ln1_pull = jax.vjp(layer_norm, x_f32, ln1_gain, ln1_bias)
        h_one = h_one_f.astype(BF16)
        qkv, mixed, stats, attn_out = attn_fwd(h_one, wcat, bqkv_col, heads_loc, hd)
        x_mid = (x_f32 + attn_out + b_o).astype(BF16)
        mid_f32 = x_mid.astype(F32)
        h_two_f, ln2_pull = jax.vjp(layer_norm, mid_f32, ln2_gain, ln2_bias)
        h_two = h_two_f.astype(BF16)
        h_two_all = gather(h_two)
        pre_act = (dot('nw,dwf->dnf', h_two, w1) + b1[:, None, :]).astype(BF16)
        hidden_f, gelu_pull = jax.vjp(gelu_tanh, pre_act.astype(F32))
        hidden = hidden_f.astype(BF16)
        mlp_out = dot('dnf,dfw->nw', hidden, w2)
        y_img = (mid_f32 + mlp_out + b_2).astype(BF16)
        y_out = to_tokens(y_img)

        d_img = lax.dynamic_index_in_dim(d_out_all, me, 0, keepdims=False)
        d_hidden = dot('nw,dfw->dnf', d_img, w2).astype(BF16)
        (d_pre_f,) = gelu_pull(d_hidden.astype(F32))
        d_pre = d_pre_f.astype(BF16)
        d_h_two = dot('dnf,dwf->nw', d_pre, w1).astype(BF16)
        d_mid_ln, g_ln2_gain, g_ln2_bias = ln2_pull(d_h_two.astype(F32))
        d_mid = (d_img.astype(F32) + d_mid_ln).astype(BF16)
        g_all, gb_part, d_h_one, gw1, grad_w_2, gb1 = layer_bwd(h_one, d_mid, wcat, qkv, mixed, stats, h_two_all, d_out_all,
                                                                w_1.T, w_2, b_1.astype(F32)[:, None], heads_loc, hd)
        grad_w_1 = gw1.T
        grad_b_1 = gb1[:, 0].astype(BF16)
        d_h_one = d_h_one.astype(BF16)
        d_in_ln, g_ln1_gain, g_ln1_bias = ln1_pull(d_h_one.astype(F32))
        gx_img = (d_mid.astype(F32) + d_in_ln).astype(BF16)
        grad_x = to_tokens(gx_img)

        vec = jnp.concatenate([jnp.stack([g_ln1_gain, g_ln1_bias, g_ln2_gain, g_ln2_bias, jnp.sum(d_mid, axis=0, dtype=F32),
                                          jnp.sum(d_img, axis=0, dtype=F32)]), gb_part.reshape(-1, width)])
        vec = group_sum(jnp.pad(vec, ((0, -vec.shape[0] % 8), (0, 0))), size)
        gb = lax.dynamic_index_in_dim(vec[6:6 + 3 * hw * size // width].reshape(-1, 3 * hw), me, 0, keepdims=False)
        grad_b_q = gb[:hw].astype(BF16).reshape(b_q.shape)
        grad_b_v = gb[2 * hw:].astype(BF16).reshape(b_v.shape)
        gq, gk, gv = (g_all[i * hw:(i + 1) * hw].T.reshape(w_q.shape) for i in range(3))
        grad_w_o = g_all[3 * hw:].reshape(w_o.shape)
        return (y_out, grad_x, vec[0], vec[1], gq, grad_b_q, gk, gv, grad_b_v, grad_w_o,
                vec[4].astype(BF16), vec[2], vec[3], grad_w_1, grad_b_1, grad_w_2, vec[5].astype(BF16))

    return jax.shard_map(layer_step, mesh=mesh, in_specs=in_specs, out_specs=out_specs, check_vma=False)
```

```python
import functools
import math
import jax
import jax.numpy as jnp
from jax import lax
from jax.experimental import pallas as pl
from jax.experimental.pallas import tpu as pltpu
from jax.sharding import PartitionSpec as P

LN_EPS = 1e-6
F32 = jnp.float32
BF16 = jnp.bfloat16
NN = (((1,), (0,)), ((), ()))
NT = (((1,), (1,)), ((), ()))
TN = (((0,), (0,)), ((), ()))
BIAS_ROWS = 16


def mm(a, b, dims):
    return lax.dot_general(a, b, dims, preferred_element_type=F32)


def push(src, dst, ssem, rsem, dev):
    return pltpu.make_async_remote_copy(src_ref=src, dst_ref=dst, send_sem=ssem, recv_sem=rsem,
                                        device_id={'tp': dev}, device_id_type=pl.DeviceIdType.MESH)


def greet_all(size):
    me = lax.axis_index('tp')
    barrier = pltpu.get_barrier_semaphore()
    for r in range(1, size):
        pl.semaphore_signal(barrier, inc=1, device_id={'tp': lax.rem(me + r, size)}, device_id_type=pl.DeviceIdType.MESH)
    pl.semaphore_wait(barrier, size - 1)


def swap_core(dev):
    return dev + 1 - 2 * lax.rem(dev, 2)


def ring(size):
    me = lax.axis_index('tp')
    return me, lax.rem(me + 2, size), lax.rem(me + size - 2, size), lax.rem(me + size // 2, size)


class Gather:
    COPIES = 14

    def __init__(self, size, src, dst, sems, off):
        me, right, left, opp = ring(size)
        partner = swap_core(me)
        plan = [(me, 0, right), (me, 1, right), (left, 0, right), (me, 1, left), (me, 0, left), (right, 1, left)]
        plan += [(owner, half, partner) for owner in (me, left, right, opp) for half in range(2)]

        def make(i):
            owner, half, dev = plan[i]
            out = dst(owner, half)
            return push(src(half) if owner is me else out, out, sems[0].at[off + i], sems[1].at[off + i], dev)

        self.copy = make

    def start(self):
        for i in (0, 3, 1, 4, 6, 7):
            self.copy(i).start()

    def forward(self):
        for got, sends in ((0, (2, 8)), (3, (5, 11))):
            self.copy(got).wait_recv()
            for i in sends:
                self.copy(i).start()

    def relay(self, *pairs):
        for got, i in pairs:
            self.copy(got).wait_recv()
            self.copy(i).start()

    def near(self):
        self.relay((1, 9), (4, 10))

    def far(self):
        self.relay((2, 12), (5, 13))

    def received(self, *which):
        for i in which:
            self.copy(i).wait_recv()

    def sent(self):
        for i in range(self.COPIES):
            self.copy(i).wait_send()

    def follow(self, step, after_forward):
        def at(k, *calls):
            @pl.when(step == k)
            def _():
                for call in calls:
                    call()

        at(1, lambda: self.received(6, 7))
        at(2, self.forward, after_forward, lambda: self.relay((1, 9)))
        at(3, lambda: self.relay((4, 10)))
        at(4, lambda: self.received(8, 9))
        at(5, lambda: self.received(10, 11))
        at(6, self.far)
        at(7, lambda: self.received(12, 13))


class Exchange:
    COPIES = 9

    def __init__(self, size, src, dst, via, sems, off):
        me, right, left, opp = ring(size)
        plan = [(src(opp), via.at[0], left), (src(swap_core(opp)), via.at[1], right)]
        plan += [(src(dev), dst(me), dev) for side in (right, left) for dev in (side, swap_core(side))]
        plan += [(src(swap_core(me)), dst(me), swap_core(me)), (via.at[0], dst(right), left), (via.at[1], dst(left), swap_core(right))]
        self.copy = lambda i: push(*plan[i][:2], sems[0].at[off + i], sems[1].at[off + i], plan[i][2])

    def start(self):
        for i in range(7):
            self.copy(i).start()

    def forward(self):
        for got, i in ((0, 7), (1, 8)):
            self.copy(got).wait_recv()
            self.copy(i).start()

    def close(self):
        for i in range(2, self.COPIES):
            self.copy(i).wait_recv()
        for i in range(self.COPIES):
            self.copy(i).wait_send()


def pair_rows(ref, c):
    return jnp.concatenate([ref[2 * c].astype(F32), ref[2 * c + 1].astype(F32)])


def pair_chunks(size, tok, body):
    pl.loop(0, size // 2)(lambda c: body(c, pl.ds(pl.multiple_of(c * 2 * tok, 16), 2 * tok)))


def cut(rows):
    half = rows // 2 // 16 * 16
    return pl.ds(0, half), pl.ds(half, rows - half)


def head(z, i, hd):
    return z[i * hd:(i + 1) * hd]


def norm_rows(z):
    centered = z - jnp.mean(z, axis=-1, keepdims=True)
    inv = lax.rsqrt(jnp.mean(centered * centered, axis=-1, keepdims=True) + LN_EPS)
    return centered * inv, inv


def norm_rows_pull(xhat, inv, dh, gain):
    dxh = dh * gain
    return inv * (dxh - jnp.mean(dxh, axis=-1, keepdims=True) - xhat * jnp.mean(dxh * xhat, axis=-1, keepdims=True))


def arrival(i, size):
    me = lax.axis_index('tp')
    partner = me + 1 - 2 * lax.rem(me, 2)
    hop = jnp.where(i < 2, 0, jnp.where(i >= 6, size // 2, jnp.where(lax.rem(i, 2) == 0, size - 2, 2)))
    base = jnp.where((i == 1) | (i == 4) | (i == 5) | (i == 7), partner, me)
    return lax.rem(base + hop, size)


def front_kernel(heads, hd, size, x_ref, wl_ref, g1_ref, c1_ref, bo_ref, g2_ref, c2_ref, w1_ref, do_ref,
                 qkv_ref, mix_ref, st_ref, h1_ref, xm_ref, h2_ref, xi_ref, wa_ref, doa_ref, w1a_ref,
                 w_all, x_all, via, acc_ref, own_do, loc_sem, out_sem, send_sem, recv_sem):
    hw = heads * hd
    scale = 1.0 / math.sqrt(hd)
    step = pl.program_id(0)
    me = lax.axis_index('tp')
    imgs, tok, width = x_ref.shape
    n = h1_ref.shape[0]
    rows = wl_ref.shape[0]
    sems = send_sem, recv_sem
    images = pl.ds(0, imgs // 2), pl.ds(imgs // 2, imgs // 2)
    mine = lambda dev: pl.ds(pl.multiple_of(dev * tok, 8), tok)
    gw = Gather(size, lambda h: wl_ref.at[cut(rows)[h]], lambda d, h: w_all.at[d, cut(rows)[h]], sems, 0)
    gw1 = Gather(size, lambda h: w1_ref.at[cut(width)[h]], lambda d, h: w1a_ref.at[d, cut(width)[h]], sems, Gather.COPIES)
    gdo = Gather(size, lambda h: do_ref.at[images[h]], lambda d, h: doa_ref.at[images[h], mine(d)], sems, 2 * Gather.COPIES)
    ex = Exchange(size, lambda d: x_ref.at[d], lambda d: x_all.at[d], via, sems, 3 * Gather.COPIES)
    local = lambda src, dst, i: pltpu.make_async_copy(src, dst, loc_sem.at[i])
    in_x, in_do = local(x_ref.at[me], x_all.at[me], 0), local(do_ref, own_do, 1)
    out_w, out_w1 = local(wl_ref, wa_ref.at[me], 2), local(w1_ref, w1a_ref.at[me], 3)
    out_x, out_do = local(x_all, xi_ref, 4), local(own_do, doa_ref.at[:, mine(me)], 5)

    def out_block(i):
        dev = arrival(i, size)
        return pltpu.make_async_copy(w_all.at[dev], wa_ref.at[dev], out_sem.at[i])

    @pl.when(step == 0)
    def _():
        for c in (in_x, in_do, out_w, out_w1):
            c.start()
        greet_all(size)
        ex.start()
        gw.start()
        w_all[me] = wl_ref[...]
        ex.forward()
        in_x.wait()
        ex.close()
        out_x.start()

        def body(c, rows):
            xhat, _ = norm_rows(pair_rows(x_all, c))
            h1_ref[rows] = (xhat * g1_ref[...] + c1_ref[...]).astype(BF16)

        pair_chunks(size, tok, body)
        in_do.wait()
        out_do.start()

    gw.follow(step, gw1.start)

    @pl.when(step > 0)
    def _():
        out_block(step).start()

    w = w_all.at[arrival(step, size)]
    bias = mm(w[4 * hw:, :3 * hw], jnp.ones((BIAS_ROWS, n), BF16), TN)
    qkv = (mm(w[:3 * hw], h1_ref[...], NT) + bias).astype(BF16)
    qkv_ref[0] = qkv
    for h in range(heads):
        q, k, v = (head(qkv, i * heads + h, hd) for i in range(3))
        s = mm(k, q, TN) * scale
        top = jnp.max(s, axis=0, keepdims=True)
        e = jnp.exp(s - top)
        inv = 1.0 / jnp.sum(e, axis=0, keepdims=True)
        st_ref[0, h:h + 1] = top
        st_ref[0, heads + h:heads + h + 1] = inv
        mix_ref[0, h * hd:(h + 1) * hd] = mm(v, (e * inv).astype(BF16), NN).astype(BF16)
    out = mm(mix_ref[0], w[3 * hw:4 * hw], TN)

    @pl.when(step == 0)
    def _():
        acc_ref[...] = out

    @pl.when(step > 0)
    def _():
        acc_ref[...] += out

    @pl.when(step == size - 1)
    def _():
        gw1.forward()
        gdo.start()

        def body(c, rows):
            mid = (pair_rows(x_all, c) + acc_ref[rows] + bo_ref[...].astype(F32)).astype(BF16)
            xm_ref[rows] = mid
            xhat, _ = norm_rows(mid.astype(F32))
            h2_ref[rows] = (xhat * g2_ref[...] + c2_ref[...]).astype(BF16)

        pair_chunks(size, tok, body)
        gw1.near()
        gw1.far()
        gdo.forward()
        gdo.near()
        gdo.far()
        for g in (gw1, gdo):
            g.received(*range(6, Gather.COPIES))
        for g in (gw, gw1, gdo):
            g.sent()
        for c in (out_x, out_w, out_w1, out_do):
            c.wait()
        for i in range(1, size):
            out_block(i).wait()


def whole(*shape):
    return pl.BlockSpec(shape, lambda i: (0,) * len(shape), pipeline_mode=pl.Buffered(1))


def block(index, *shape):
    return pl.BlockSpec((1,) + shape, lambda i: (index(i),) + (0,) * len(shape))


def dma(k):
    return pltpu.SemaphoreType.DMA((k,))


def kernel_params(collective_id):
    return pltpu.CompilerParams(dimension_semantics=("arbitrary",), vmem_limit_bytes=67_043_328,
                                collective_id=collective_id, has_side_effects=True)


ANY = pl.BlockSpec(memory_space=pl.ANY)


def front(x, wloc, ln1_gain, ln1_bias, b_o, ln2_gain, ln2_bias, w_1, d_out, heads, hd):
    rows, width = wloc.shape
    imgs, tok, _ = x.shape
    size = imgs
    n = size * tok
    hw = heads * hd
    order = lambda i: arrival(i, size)
    row = whole(1, width)
    bf = lambda *shape: jax.ShapeDtypeStruct(shape, BF16)
    copies = 3 * Gather.COPIES + Exchange.COPIES
    return pl.pallas_call(
        functools.partial(front_kernel, heads, hd, size),
        grid=(size,),
        in_specs=[ANY, whole(rows, width), row, row, row, row, row, whole(*w_1.shape), ANY],
        out_specs=[block(order, 3 * hw, n), block(order, hw, n), block(order, 2 * heads, n),
                   whole(n, width), whole(n, width), whole(n, width), ANY, ANY, ANY, ANY],
        out_shape=[bf(size, 3 * hw, n), bf(size, hw, n), jax.ShapeDtypeStruct((size, 2 * heads, n), F32), bf(n, width), bf(n, width),
                   bf(n, width), bf(size, tok, width), bf(size, rows, width), bf(imgs, n, width), bf(size, *w_1.shape)],
        scratch_shapes=[pltpu.VMEM((size, rows, width), BF16), pltpu.VMEM((size, tok, width), BF16), pltpu.VMEM((2, tok, width), BF16),
                        pltpu.VMEM((n, width), F32), pltpu.VMEM(d_out.shape, BF16), dma(6), dma(size), dma(copies), dma(copies)],
        compiler_params=kernel_params(1),
        name="front",
    )(x, wloc, ln1_gain[None], ln1_bias[None], b_o[None], ln2_gain[None], ln2_bias[None], w_1, d_out)


def gelu_and_slope(u):
    c = math.sqrt(2.0 / math.pi)
    u2 = u * u
    t = jnp.tanh(c * (u + 0.044715 * (u2 * u)))
    half = 0.5 * (1.0 + t)
    slope = half + 0.5 * u * (1.0 - t * t) * (c * (1.0 + (3.0 * 0.044715) * u2))
    return u * half, slope


def block_of_step(j, size):
    me = lax.axis_index('tp')
    chips = size // 2
    off = jnp.where(j < 2, 2, jnp.where(j < 4, 1, jnp.where(j < 6, 3, 0)))
    chip = lax.rem(lax.div(me, 2) + off, chips)
    core = lax.rem(me, 2)
    side = jnp.where(lax.rem(j, 2) == 0, 1 - core, core)
    return 2 * chip + side


def back_kernel(heads, hd, size, h2_ref, xm_ref, dself_ref, w1b_ref, b_ref, w2_ref, g2_ref, b2_ref,
                h_ref, w_ref, qkv_ref, mix_ref, st_ref, do_ref, w1_ref, b1_ref, x3_ref, gain_ref,
                g_ref, gw1_ref, gw2_ref, gb1_ref, gx_ref, vec_ref, yo_ref, h2a_ref, w2a_ref,
                w2_buf, dm_ref, dm3_ref, y3_ref, h_buf, dqkv_ref, dh_ref, gx_own, v_own, v_all, via_y, via_g,
                outs, pair_in, opp_l, opp_r, near_l, near_r, acc, loc_sem, h_sem, send_sem, recv_sem):
    hw = heads * hd
    half = 2 * hw
    scale = 1.0 / math.sqrt(hd)
    step = pl.program_id(0)
    j = step - size
    m = j - size
    me, right, left, _ = ring(size)
    partner = swap_core(me)
    n, width = h_ref.shape
    rows = outs.shape[1]
    tok = x3_ref.shape[1]
    mlp = w2_ref.shape[0]
    sems = send_sem, recv_sem
    own = 2
    gw2 = Gather(size, lambda h: w2_ref.at[cut(mlp)[h]], lambda d, h: w2a_ref.at[d, cut(mlp)[h]], sems, 0)
    gh2 = Gather(size, lambda h: h2_ref.at[cut(n)[h]], lambda d, h: h2a_ref.at[d, cut(n)[h]], sems, Gather.COPIES)
    base = 2 * Gather.COPIES
    ex_y = Exchange(size, lambda d: y3_ref.at[d], lambda d: yo_ref.at[d], via_y, sems, base)
    base += Exchange.COPIES
    ex_g = Exchange(size, lambda d: gx_own.at[d], lambda d: gx_ref.at[d], via_g, sems, base)
    base += Exchange.COPIES
    local = lambda src, dst, i: pltpu.make_async_copy(src, dst, loc_sem.at[i])
    out_h2 = local(h2_ref, h2a_ref.at[me], 0)
    y_local, gx_local = local(y3_ref.at[me], yo_ref.at[me], 1), local(gx_own.at[me], gx_ref.at[me], 2)

    def numbered(src, dst, i, dev):
        return push(src, dst, send_sem.at[base + i], recv_sem.at[base + i], dev)

    def pair_copy(t):
        return numbered(outs.at[t % own], pair_in.at[t % own], t, partner)

    pairs = size // 2
    lo, hi = pl.ds(0, half), pl.ds(half, rows - half)
    one, two = own + 1, own + 2
    opp_right = lambda: numbered(outs.at[own, lo], opp_l, pairs, right)
    opp_left = lambda: numbered(outs.at[own, hi], opp_r, pairs + 1, left)
    right_hi = lambda: numbered(outs.at[one, hi], near_l.at[hi], pairs + 2, right)
    right_lo = lambda: numbered(outs.at[one, lo], near_l.at[lo], pairs + 3, right)
    left_lo = lambda: numbered(outs.at[two, lo], near_r.at[lo], pairs + 4, left)
    left_hi = lambda: numbered(outs.at[two, hi], near_r.at[hi], pairs + 5, left)

    def v_copy(dev, slot):
        return push(v_own, v_all.at[slot], send_sem.at[base + 2 * size + dev], recv_sem.at[base + 2 * size + slot], dev)

    def h_copy(i):
        slot = lax.rem(i, 2)
        return pltpu.make_async_copy(h2a_ref.at[i], h_buf.at[slot], h_sem.at[slot])

    @pl.when(step == 0)
    def _():
        out_h2.start()
        greet_all(size)
        gw2.start()
        w2_buf[...] = w2_ref[...]

    gw2.follow(step, gh2.start)

    @pl.when(step < size)
    def _():
        @pl.when(step > 0)
        def _():
            c = local(w2a_ref.at[arrival(step, size)], w2_buf, 3)
            c.start()
            c.wait()

        w2 = w2_buf[...]
        u = (mm(h2_ref[...], w1b_ref[0], NN) + b_ref[0, 0:1, 3 * hw:3 * hw + mlp].astype(F32)).astype(BF16).astype(F32)
        dg = mm(dself_ref[0], w2, NT).astype(BF16).astype(F32)
        g, slope = gelu_and_slope(u)
        ypart = mm(g.astype(BF16), w2, NN)
        dpart = mm((dg * slope).astype(BF16), w1b_ref[0], NT)

        @pl.when(step == 0)
        def _():
            acc[:n] = ypart
            dh_ref[...] = dpart

        @pl.when(step > 0)
        def _():
            acc[:n] += ypart
            dh_ref[...] += dpart

    @pl.when(j == -1)
    def _():
        v_own[...] = jnp.zeros_like(v_own)

        def body(c, part):
            mid = xm_ref[part].astype(F32)
            y = mid + acc[part] + b2_ref[...].astype(F32)
            xhat, inv = norm_rows(mid)
            dh = dh_ref[part].astype(BF16).astype(F32)
            do = dself_ref[0, part].astype(F32)
            dm = do + norm_rows_pull(xhat, inv, dh, g2_ref[...])
            dm_ref[part] = dm.astype(BF16)
            for side in range(2):
                tokens = slice(side * tok, (side + 1) * tok)
                y3_ref[2 * c + side] = y[tokens].astype(BF16)
                dm3_ref[2 * c + side] = dm[tokens].astype(BF16)
            for i, v in enumerate((dh * xhat, dh, dm.astype(BF16).astype(F32), do)):
                v_own[2 + i:3 + i] += jnp.sum(v, axis=0, keepdims=True)

        pair_chunks(size, tok, body)
        gw2.sent()
        gh2.forward()

    @pl.when((j >= 0) & (j < size))
    def _():
        d_mix = mm(w_ref[0, 3 * hw:4 * hw], dm_ref[...], NT).astype(BF16)
        qkv = qkv_ref[0]
        for h in range(heads):
            q, k, v = (head(qkv, i * heads + h, hd) for i in range(3))
            da = head(d_mix, h, hd)
            s = mm(k, q, TN) * scale
            p = jnp.exp(s - st_ref[0, h:h + 1]) * st_ref[0, heads + h:heads + h + 1]
            dp = mm(v, da, TN).astype(BF16).astype(F32)
            ds = (p * (dp - jnp.sum(p * dp, axis=0, keepdims=True)) * scale).astype(BF16)
            for i, z in enumerate((mm(k, ds, NN), mm(q, ds, NT), mm(da, p.astype(BF16), NT))):
                at = i * hw + h * hd
                dqkv_ref[at:at + hd] = z.astype(BF16)
        dqkv = dqkv_ref[...]
        part = mm(dqkv, w_ref[0, :3 * hw], TN)

        @pl.when(j == 0)
        def _():
            dh_ref[...] = part

        @pl.when(j > 0)
        def _():
            dh_ref[...] += part

        for t in range(own, pairs):
            @pl.when(j == 2 * t)
            def _():
                pair_copy(t - own).wait_send()

        @pl.when(j == size - 1)
        def _():
            opp_right().wait_send()
            opp_left().wait_send()

        turn = lax.div(j, 2)
        out = outs.at[jnp.where(lax.rem(j, 2) == 0, lax.rem(turn, own), own + lax.rem(turn, pairs - 1))]
        out[:3 * hw] = mm(dqkv, h_ref[...], NN)
        out[3 * hw:4 * hw] = mm(mix_ref[0], dm_ref[...], NN)
        sums = mm(jnp.ones((BIAS_ROWS, n), BF16), dqkv, NT)
        out[4 * hw:] = jnp.concatenate([sums, jnp.zeros((BIAS_ROWS, width - 3 * hw), F32)], axis=1)

        for t in range(pairs):
            @pl.when(j == 2 * t)
            def _():
                pair_copy(t).start()

            @pl.when(j == 2 * t + 1)
            def _():
                pair_copy(t).wait_recv()
                outs[own + t % (pairs - 1)] += pair_in[t % own]

        @pl.when(j == 1)
        def _():
            opp_right().start()
            opp_left().start()

        @pl.when(j == 3)
        def _():
            right_hi().start()
            gh2.near()

        @pl.when(j == 5)
        def _():
            left_lo().start()

        @pl.when(j == size - 2)
        def _():
            gh2.far()

        @pl.when(j == size - 1)
        def _():
            opp_right().wait_recv()
            outs[one, lo] += opp_l[...]
            right_lo().start()
            opp_left().wait_recv()
            outs[two, hi] += opp_r[...]
            left_hi().start()
            ex_y.start()
            y_local.start()

    @pl.when(m == 0)
    def _():
        gh2.received(*range(6, Gather.COPIES))
        out_h2.wait()
        h_copy(0).start()

        @pl.loop(0, size)
        def _(dev):
            dh = dh_ref[pl.ds(pl.multiple_of(dev * tok, 8), tok)].astype(BF16).astype(F32)
            xhat, inv = norm_rows(x3_ref[dev].astype(F32))
            gx_own[dev] = (dm3_ref[dev].astype(F32) + norm_rows_pull(xhat, inv, dh, gain_ref[...])).astype(BF16)
            v_own[0:1] += jnp.sum(dh * xhat, axis=0, keepdims=True)
            v_own[1:2] += jnp.sum(dh, axis=0, keepdims=True)

        for r in range(1, size):
            v_copy(lax.rem(me + r, size), me).start()
        ex_g.start()
        gx_local.start()
        v_all[me] = v_own[...]

    @pl.when(m >= 0)
    def _():
        h_copy(m).wait()

        @pl.when(m < size - 1)
        def _():
            h_copy(m + 1).start()

        h2 = h_buf[lax.rem(m, 2)]
        do = do_ref[0]
        u = (mm(w1_ref[...], h2, NT) + b1_ref[...]).astype(BF16).astype(F32)
        dg = mm(w2_ref[...], do, NT).astype(BF16).astype(F32)
        g, slope = gelu_and_slope(u)
        du = (dg * slope).astype(BF16)
        g1 = mm(du, h2, NN)
        g2 = mm(g.astype(BF16), do, NN)
        gb = jnp.sum(du.astype(F32), axis=1, keepdims=True)

        @pl.when(m == 0)
        def _():
            acc[:mlp] = g1
            acc[mlp:] = g2
            gb1_ref[...] = gb

        @pl.when(m > 0)
        def _():
            acc[:mlp] += g1
            acc[mlp:] += g2
            gb1_ref[...] += gb

    @pl.when(m == size - 1)
    def _():
        gw1_ref[...] = acc[:mlp].astype(BF16)
        gw2_ref[...] = acc[mlp:].astype(BF16)
        ring_copies = (right_hi(), right_lo(), left_lo(), left_hi())
        for c in ring_copies:
            c.wait_recv()
        ex_y.forward()
        ex_g.forward()
        g_ref[...] = (outs[own] + near_l[...] + near_r[...]).astype(BF16)
        for c in ring_copies + (pair_copy(pairs - 2), pair_copy(pairs - 1)):
            c.wait_send()
        gh2.sent()
        for r in range(1, size):
            dev = lax.rem(me + r, size)
            v_copy(dev, dev).wait()
        total = v_all[0]
        for i in range(1, size):
            total += v_all[i]
        vec_ref[...] = total
        ex_y.close()
        ex_g.close()
        gx_local.wait()
        y_local.wait()


def back(h_two, x_mid, d_out_all, w1_all, wcat, w_2, gain2, b_2, h_one, qkv, mix, stats, w1t, b1_col, x3, gain1, heads, hd):
    size, rows, width = wcat.shape
    n = h_one.shape[0]
    mlp = w_2.shape[0]
    hw = heads * hd
    first = lambda i: arrival(jnp.minimum(i, size - 1), size)
    second = lambda i: block_of_step(jnp.clip(i - size, 0, size - 1), size)
    third = lambda i: jnp.maximum(i - 2 * size, 0)
    buf = lambda *shape: pltpu.VMEM(shape, F32)
    half_buf = lambda *shape: pltpu.VMEM(shape, BF16)
    bf = lambda *shape: jax.ShapeDtypeStruct(shape, BF16)
    row = whole(1, width)
    copies = 2 * Gather.COPIES + 2 * Exchange.COPIES + 3 * size
    half = 2 * hw
    tokens = x3.shape[1:]
    return pl.pallas_call(
        functools.partial(back_kernel, heads, hd, size),
        grid=(3 * size,),
        in_specs=[whole(n, width), whole(n, width),
                  pl.BlockSpec((1, n, width), lambda i: (lax.axis_index('tp'), 0, 0), pipeline_mode=pl.Buffered(1)),
                  block(first, width, mlp),
                  pl.BlockSpec((1, BIAS_ROWS, width), lambda i: (first(i), rows // BIAS_ROWS - 1, 0)),
                  whole(mlp, width), row, row,
                  whole(n, width), block(second, rows, width), block(second, 3 * hw, n), block(second, hw, n), block(second, 2 * heads, n),
                  block(third, n, width), whole(mlp, width), whole(mlp, 1), whole(*x3.shape), row],
        out_specs=[whole(rows, width), whole(mlp, width), whole(mlp, width), whole(mlp, 1), ANY, whole(8, width), ANY, ANY, ANY],
        out_shape=[bf(rows, width), bf(mlp, width), bf(mlp, width), jax.ShapeDtypeStruct((mlp, 1), F32), bf(*x3.shape),
                   jax.ShapeDtypeStruct((8, width), F32), bf(*x3.shape), bf(size, n, width), bf(size, mlp, width)],
        scratch_shapes=[half_buf(mlp, width), half_buf(n, width), half_buf(*x3.shape), half_buf(*x3.shape), half_buf(2, n, width),
                        half_buf(3 * hw, n), buf(n, width), half_buf(*x3.shape), buf(8, width), buf(size, 8, width),
                        half_buf(2, *tokens), half_buf(2, *tokens), buf(size // 2 + 1, rows, width), buf(2, rows, width),
                        buf(half, width), buf(rows - half, width), buf(rows, width), buf(rows, width), buf(2 * mlp, width),
                        dma(4), dma(2), dma(copies), dma(copies)],
        compiler_params=kernel_params(2),
        name="back",
    )(h_two, x_mid, d_out_all, w1_all, wcat, w_2, gain2[None], b_2[None], h_one, wcat, qkv, mix, stats, d_out_all, w1t, b1_col,
      x3, gain1[None])


def solution(mesh):
    act_spec = P('dp', 'tp', None)
    replicated = P()
    head_w = P(None, 'tp', None)
    head_b = P('tp', None)
    grad_head_w = P('dp', 'tp', None)
    grad_head_b = P(('dp', 'tp'), None)
    grad_vec = P('dp')
    in_specs = (act_spec, act_spec, replicated, replicated, head_w, head_b, head_w, head_w, head_b,
                P('tp', None, None), replicated, replicated, replicated, P(None, 'tp'), P('tp'), P('tp', None), replicated)
    out_specs = (act_spec, act_spec, grad_vec, grad_vec, grad_head_w, grad_head_b, grad_head_w, grad_head_w, grad_head_b,
                 P(('dp', 'tp'), None, None), grad_vec, grad_vec, grad_vec, P('dp', 'tp'), P(('dp', 'tp')),
                 P(('dp', 'tp'), None), grad_vec)

    def layer_step(x, d_out, ln1_gain, ln1_bias, w_q, b_q, w_k, w_v, b_v, w_o, b_o, ln2_gain, ln2_bias, w_1, b_1, w_2, b_2):
        width = x.shape[-1]
        heads_loc, hd = w_q.shape[1:]
        hw = heads_loc * hd
        flat = lambda w: w.reshape(width, hw).T
        bias_row = jnp.concatenate([b_q.reshape(hw), jnp.zeros((hw,), BF16), b_v.reshape(hw), b_1])
        bias_rows = jnp.zeros((BIAS_ROWS, width), BF16).at[0, :bias_row.shape[0]].set(bias_row)
        wloc = jnp.concatenate([flat(w_q), flat(w_k), flat(w_v), w_o.reshape(hw, width), bias_rows])
        qkv, mixed, stats, h_one, x_mid, h_two, x_img, wcat, d_out_all, w1_all = front(
            x, wloc, ln1_gain, ln1_bias, b_o, ln2_gain, ln2_bias, w_1, d_out, heads_loc, hd)
        g_all, gw1, grad_w_2, gb1, grad_x, vec, y_out, _, _ = back(
            h_two, x_mid, d_out_all, w1_all, wcat, w_2, ln2_gain, b_2, h_one, qkv, mixed, stats, w_1.T,
            b_1.astype(F32)[:, None], x_img, ln1_gain, heads_loc, hd)
        grad_w_1 = gw1.T
        grad_b_1 = gb1[:, 0].astype(BF16)
        gb = g_all[4 * hw, :3 * hw]
        grad_b_q = gb[:hw].reshape(b_q.shape)
        grad_b_v = gb[2 * hw:].reshape(b_v.shape)
        gq, gk, gv = (g_all[i * hw:(i + 1) * hw].T.reshape(w_q.shape) for i in range(3))
        grad_w_o = g_all[3 * hw:4 * hw].reshape(w_o.shape)
        return (y_out, grad_x, vec[0], vec[1], gq, grad_b_q, gk, gv, grad_b_v, grad_w_o,
                vec[4].astype(BF16), vec[2], vec[3], grad_w_1, grad_b_1, grad_w_2, vec[5].astype(BF16))

    return jax.shard_map(layer_step, mesh=mesh, in_specs=in_specs, out_specs=out_specs, check_vma=False)
```

```python
import functools
import math
import jax
import jax.numpy as jnp
from jax import lax
from jax.experimental import pallas as pl
from jax.experimental.pallas import tpu as pltpu
from jax.sharding import PartitionSpec as P

LN_EPS = 1e-6
F32 = jnp.float32
BF16 = jnp.bfloat16
NN = (((1,), (0,)), ((), ()))
NT = (((1,), (1,)), ((), ()))
TN = (((0,), (0,)), ((), ()))
BIAS_ROWS = 16


def mm(a, b, dims):
    return lax.dot_general(a, b, dims, preferred_element_type=F32)


def push(src, dst, ssem, rsem, dev):
    return pltpu.make_async_remote_copy(src_ref=src, dst_ref=dst, send_sem=ssem, recv_sem=rsem,
                                        device_id={'tp': dev}, device_id_type=pl.DeviceIdType.MESH)


def greet_all(size):
    me = lax.axis_index('tp')
    barrier = pltpu.get_barrier_semaphore()
    for r in range(1, size):
        pl.semaphore_signal(barrier, inc=1, device_id={'tp': lax.rem(me + r, size)}, device_id_type=pl.DeviceIdType.MESH)
    pl.semaphore_wait(barrier, size - 1)


def swap_core(dev):
    return dev + 1 - 2 * lax.rem(dev, 2)


def ring(size):
    me = lax.axis_index('tp')
    return me, lax.rem(me + 2, size), lax.rem(me + size - 2, size), lax.rem(me + size // 2, size)


class Gather:
    COPIES = 14

    def __init__(self, size, src, dst, sems, off):
        me, right, left, opp = ring(size)
        partner = swap_core(me)
        plan = [(me, 0, right), (me, 1, right), (left, 0, right), (me, 1, left), (me, 0, left), (right, 1, left)]
        plan += [(owner, half, partner) for owner in (me, left, right, opp) for half in range(2)]

        def make(i):
            owner, half, dev = plan[i]
            out = dst(owner, half)
            return push(src(half) if owner is me else out, out, sems[0].at[off + i], sems[1].at[off + i], dev)

        self.copy = make

    def start(self):
        for i in (0, 3, 1, 4, 6, 7):
            self.copy(i).start()

    def forward(self):
        for got, sends in ((0, (2, 8)), (3, (5, 11))):
            self.copy(got).wait_recv()
            for i in sends:
                self.copy(i).start()

    def relay(self, *pairs):
        for got, i in pairs:
            self.copy(got).wait_recv()
            self.copy(i).start()

    def near(self):
        self.relay((1, 9), (4, 10))

    def far(self):
        self.relay((2, 12), (5, 13))

    def received(self, *which):
        for i in which:
            self.copy(i).wait_recv()

    def sent(self):
        for i in range(self.COPIES):
            self.copy(i).wait_send()

    def follow(self, step, *ahead):
        def at(k, *calls):
            @pl.when(step == k)
            def _():
                for call in calls:
                    call()

        at(1, lambda: self.received(6, 7))
        at(2, *ahead, lambda: self.relay((1, 9)))
        at(3, lambda: self.relay((4, 10)))
        at(4, lambda: self.received(8, 9))
        at(5, lambda: self.received(10, 11))
        at(6, self.far)
        at(7, lambda: self.received(12, 13))


class Exchange:
    COPIES = 9

    def __init__(self, size, src, dst, via, sems, off):
        me, right, left, opp = ring(size)
        plan = [(src(opp), via.at[0], left), (src(swap_core(opp)), via.at[1], right)]
        plan += [(src(dev), dst(me), dev) for side in (right, left) for dev in (side, swap_core(side))]
        plan += [(src(swap_core(me)), dst(me), swap_core(me)), (via.at[0], dst(right), left), (via.at[1], dst(left), swap_core(right))]
        self.copy = lambda i: push(*plan[i][:2], sems[0].at[off + i], sems[1].at[off + i], plan[i][2])

    def start(self):
        for i in range(7):
            self.copy(i).start()

    def forward(self):
        for got, i in ((0, 7), (1, 8)):
            self.copy(got).wait_recv()
            self.copy(i).start()

    def close(self):
        for i in range(2, self.COPIES):
            self.copy(i).wait_recv()
        for i in range(self.COPIES):
            self.copy(i).wait_send()


def pair_rows(ref, c):
    return jnp.concatenate([ref[2 * c].astype(F32), ref[2 * c + 1].astype(F32)])


def pair_chunks(size, tok, body):
    pl.loop(0, size // 2)(lambda c: body(c, pl.ds(pl.multiple_of(c * 2 * tok, 16), 2 * tok)))


def cut(rows):
    half = rows // 2 // 16 * 16
    return pl.ds(0, half), pl.ds(half, rows - half)


def head(z, i, hd):
    return z[i * hd:(i + 1) * hd]


def norm_rows(z):
    centered = z - jnp.mean(z, axis=-1, keepdims=True)
    inv = lax.rsqrt(jnp.mean(centered * centered, axis=-1, keepdims=True) + LN_EPS)
    return centered * inv, inv


def norm_rows_pull(xhat, inv, dh, gain):
    dxh = dh * gain
    return inv * (dxh - jnp.mean(dxh, axis=-1, keepdims=True) - xhat * jnp.mean(dxh * xhat, axis=-1, keepdims=True))


def arrival(i, size):
    me = lax.axis_index('tp')
    partner = me + 1 - 2 * lax.rem(me, 2)
    hop = jnp.where(i < 2, 0, jnp.where(i >= 6, size // 2, jnp.where(lax.rem(i, 2) == 0, size - 2, 2)))
    base = jnp.where((i == 1) | (i == 4) | (i == 5) | (i == 7), partner, me)
    return lax.rem(base + hop, size)


def gelu_and_slope(u):
    c = math.sqrt(2.0 / math.pi)
    u2 = u * u
    t = jnp.tanh(c * (u + 0.044715 * (u2 * u)))
    half = 0.5 * (1.0 + t)
    slope = half + 0.5 * u * (1.0 - t * t) * (c * (1.0 + (3.0 * 0.044715) * u2))
    return u * half, slope


def front_kernel(heads, hd, size, x_ref, wq_ref, wk_ref, wv_ref, wo_ref, bq_ref, bv_ref, b1_ref,
                 g1_ref, c1_ref, g2_ref, c2_ref, bo_ref, b2_ref, w1_ref, w2_ref, do_ref,
                 qkv_ref, mix_ref, st_ref, h1_ref, y_ref, dm_ref, sums_ref, w1t_ref, xi_ref, wa_ref, doa_ref, h2a_ref,
                 wl_ref, w_all, w1_all, w2_all, x_all, via, acc_ref, dacc, own_do, d_img, xm_ref, h2_ref, loc_sem, out_sem, send_sem, recv_sem):
    hw = heads * hd
    scale = 1.0 / math.sqrt(hd)
    step = pl.program_id(0)
    k = step - size
    mlp = w2_ref.shape[0]
    me = lax.axis_index('tp')
    imgs, tok, width = x_ref.shape
    n = h1_ref.shape[0]
    g1, c1, g2, c2 = g1_ref[...], c1_ref[...], g2_ref[...], c2_ref[...]
    bo, b2 = (r[...].astype(F32).reshape(1, width) for r in (bo_ref, b2_ref))
    rows = wl_ref.shape[0]
    sems = send_sem, recv_sem
    images = pl.ds(0, imgs // 2), pl.ds(imgs // 2, imgs // 2)
    mine = lambda dev: pl.ds(pl.multiple_of(dev * tok, 8), tok)
    gw = Gather(size, lambda h: wl_ref.at[cut(rows)[h]], lambda d, h: w_all.at[d, cut(rows)[h]], sems, 0)
    gw1 = Gather(size, lambda h: w1_ref.at[cut(width)[h]], lambda d, h: w1_all.at[d, cut(width)[h]], sems, Gather.COPIES)
    gdo = Gather(size, lambda h: do_ref.at[images[h]], lambda d, h: doa_ref.at[images[h], mine(d)], sems, 2 * Gather.COPIES)
    gw2 = Gather(size, lambda h: w2_ref.at[cut(mlp)[h]], lambda d, h: w2_all.at[d, cut(mlp)[h]], sems, 3 * Gather.COPIES)
    gh2 = Gather(size, lambda h: h2_ref.at[cut(n)[h]], lambda d, h: h2a_ref.at[d, cut(n)[h]], sems, 4 * Gather.COPIES)
    ex = Exchange(size, lambda d: x_ref.at[d], lambda d: x_all.at[d], via, sems, 5 * Gather.COPIES)
    local = lambda src, dst, i: pltpu.make_async_copy(src, dst, loc_sem.at[i])
    in_x, in_do = local(x_ref.at[me], x_all.at[me], 0), local(do_ref, own_do, 1)
    out_w, out_h2 = local(wl_ref, wa_ref.at[me], 2), local(h2_ref, h2a_ref.at[me], 3)
    in_img = local(doa_ref.at[me], d_img, 6)
    out_x, out_do = local(x_all, xi_ref, 4), local(own_do, doa_ref.at[:, mine(me)], 5)

    def out_block(i):
        dev = arrival(i, size)
        return pltpu.make_async_copy(w_all.at[dev], wa_ref.at[dev], out_sem.at[i])

    @pl.when(step == 0)
    def _():
        in_x.start()
        in_do.start()
        greet_all(size)
        ex.start()
        for i, part in enumerate((wq_ref, wk_ref, wv_ref, wo_ref)):
            wl_ref[i * hw:(i + 1) * hw] = part[...]
        zeros = jnp.zeros((1, hw), F32)
        pieces = [r[h:h + 1].astype(F32) for r in (bq_ref, bv_ref) for h in range(heads)]
        line = jnp.concatenate(pieces[:heads] + [zeros] + pieces[heads:] + [b1_ref[...].astype(F32).reshape(1, mlp)]
                               + [zeros] * ((width - 3 * hw - mlp) // hw), axis=1)
        wl_ref[4 * hw:] = jnp.where(lax.broadcasted_iota(jnp.int32, (BIAS_ROWS, width), 0) == 0, line, 0.0).astype(BF16)
        ex.forward()
        gw.start()
        out_w.start()
        w_all[me] = wl_ref[...]
        in_x.wait()
        ex.close()
        out_x.start()

        def body(c, rows):
            xhat, _ = norm_rows(pair_rows(x_all, c))
            h1_ref[rows] = (xhat * g1 + c1).astype(BF16)

        pair_chunks(size, tok, body)
        in_do.wait()
        out_do.start()

    gw.follow(step, gw.forward, gdo.start)

    @pl.when((step > 0) & (k < 0))
    def _():
        out_block(step).start()

    @pl.when(k < 0)
    def _():
        w = w_all.at[arrival(step, size)]
        bias = mm(w[4 * hw:, :3 * hw], jnp.ones((BIAS_ROWS, n), BF16), TN)
        qkv = (mm(w[:3 * hw], h1_ref[...], NT) + bias).astype(BF16)
        qkv_ref[0] = qkv
        for h in range(heads):
            q, key, v = (head(qkv, i * heads + h, hd) for i in range(3))
            s = mm(key, q, TN) * scale
            top = jnp.max(s, axis=0, keepdims=True)
            e = jnp.exp(s - top)
            inv = 1.0 / jnp.sum(e, axis=0, keepdims=True)
            st_ref[0, h:h + 1] = top
            st_ref[0, heads + h:heads + h + 1] = inv
            mix_ref[0, h * hd:(h + 1) * hd] = mm(v, (e * inv).astype(BF16), NN).astype(BF16)
        out = mm(mix_ref[0], w[3 * hw:4 * hw], TN)

        @pl.when(step == 0)
        def _():
            acc_ref[...] = out

        @pl.when(step > 0)
        def _():
            acc_ref[...] += out

    @pl.when(k == -1)
    def _():
        gdo.forward()
        gw1.start()

        def body(c, rows):
            mid = (pair_rows(x_all, c) + acc_ref[rows] + bo).astype(BF16)
            xm_ref[rows] = mid
            xhat, _ = norm_rows(mid.astype(F32))
            h2_ref[rows] = (xhat * g2 + c2).astype(BF16)

        pair_chunks(size, tok, body)

    @pl.when(k == 0)
    def _():
        out_h2.start()
        w1_all[me] = w1_ref[...]
        w2_all[me] = w2_ref[...]
        w1t_ref[...] = w1_ref[...].T
        gdo.near()
        gdo.far()
        gw1.forward()
        gw2.start()
        gdo.received(*range(6, Gather.COPIES))
        out_do.wait()
        in_img.start()
        in_img.wait()

    gw1.follow(k)
    gw2.follow(k, gw2.forward, gh2.start)

    @pl.when(k >= 0)
    def _():
        dev = arrival(k, size)
        w1, w2 = w1_all[dev], w2_all[dev]
        b1 = w_all[dev, 4 * hw:4 * hw + 1, 3 * hw:3 * hw + mlp].astype(F32)
        u = (mm(h2_ref[...], w1, NN) + b1).astype(BF16).astype(F32)
        dg = mm(d_img[...], w2, NT).astype(BF16).astype(F32)
        g, slope = gelu_and_slope(u)
        ypart = mm(g.astype(BF16), w2, NN)
        dpart = mm((dg * slope).astype(BF16), w1, NT)

        @pl.when(k == 0)
        def _():
            acc_ref[...] = ypart
            dacc[...] = dpart

        @pl.when(k > 0)
        def _():
            acc_ref[...] += ypart
            dacc[...] += dpart

    @pl.when(k == size - 1)
    def _():
        sums_ref[...] = jnp.zeros_like(sums_ref)

        def body(c, part):
            mid = xm_ref[part].astype(F32)
            y_ref[part] = (mid + acc_ref[part] + b2).astype(BF16)
            xhat, inv = norm_rows(mid)
            dh = dacc[part].astype(BF16).astype(F32)
            do = d_img[part].astype(F32)
            dm = (do + norm_rows_pull(xhat, inv, dh, g2)).astype(BF16)
            dm_ref[part] = dm
            for i, v in enumerate((dh * xhat, dh, dm.astype(F32), do)):
                sums_ref[2 + i:3 + i] += jnp.sum(v, axis=0, keepdims=True)

        pair_chunks(size, tok, body)
        gh2.forward()
        gh2.near()
        gh2.far()
        gh2.received(*range(6, Gather.COPIES))
        for g in (gw, gw1, gdo, gw2, gh2):
            g.sent()
        for c in (out_x, out_w, out_h2):
            c.wait()
        for i in range(1, size):
            out_block(i).wait()


def whole(*shape):
    return pl.BlockSpec(shape, lambda i: (0,) * len(shape), pipeline_mode=pl.Buffered(1))


def block(index, *shape):
    return pl.BlockSpec((1,) + shape, lambda i: (index(i),) + (0,) * len(shape))


def dma(k):
    return pltpu.SemaphoreType.DMA((k,))


def kernel_params(collective_id):
    return pltpu.CompilerParams(dimension_semantics=("arbitrary",), vmem_limit_bytes=67_043_328,
                                collective_id=collective_id, has_side_effects=True)


ANY = pl.BlockSpec(memory_space=pl.ANY)


def front(x, weights, biases, gains, sums_bias, w_1, w_2, d_out, heads, hd):
    imgs, tok, width = x.shape
    size = imgs
    n = size * tok
    hw = heads * hd
    mlp = w_2.shape[0]
    rows = 4 * hw + BIAS_ROWS
    order = lambda i: arrival(jnp.minimum(i, size - 1), size)
    bf = lambda *shape: jax.ShapeDtypeStruct(shape, BF16)
    buf = lambda *shape: pltpu.VMEM(shape, BF16)
    copies = 5 * Gather.COPIES + Exchange.COPIES
    return pl.pallas_call(
        functools.partial(front_kernel, heads, hd, size),
        grid=(2 * size,),
        in_specs=[ANY] + [whole(*z.shape) for z in weights + biases + gains + sums_bias] + [ whole(width, mlp), whole(mlp, width), ANY],
        out_specs=[block(order, 3 * hw, n), block(order, hw, n), block(order, 2 * heads, n), whole(n, width), whole(n, width),
                   whole(n, width), whole(8, width), whole(mlp, width), ANY, ANY, ANY, ANY],
        out_shape=[bf(size, 3 * hw, n), bf(size, hw, n), jax.ShapeDtypeStruct((size, 2 * heads, n), F32), bf(n, width), bf(n, width),
                   bf(n, width), jax.ShapeDtypeStruct((8, width), F32), bf(mlp, width),
                   bf(size, tok, width), bf(size, rows, width), bf(imgs, n, width), bf(size, n, width)],
        scratch_shapes=[buf(rows, width), buf(size, rows, width), buf(size, width, mlp), buf(size, mlp, width), buf(size, tok, width), buf(2, tok, width),
                        pltpu.VMEM((n, width), F32), pltpu.VMEM((n, width), F32), buf(*d_out.shape), buf(n, width), buf(n, width),
                        buf(n, width), dma(7), dma(size), dma(copies), dma(copies)],
        compiler_params=kernel_params(1),
        name="front",
    )(x, *weights, *biases, *gains, *sums_bias, w_1, w_2, d_out)


def block_of_step(j, size):
    me = lax.axis_index('tp')
    chips = size // 2
    off = jnp.where(j < 2, 2, jnp.where(j < 4, 1, jnp.where(j < 6, 3, 0)))
    chip = lax.rem(lax.div(me, 2) + off, chips)
    core = lax.rem(me, 2)
    side = jnp.where(lax.rem(j, 2) == 0, 1 - core, core)
    return 2 * chip + side


def back_kernel(heads, hd, size, h_ref, dm_ref, w_ref, qkv_ref, mix_ref, st_ref, h2_ref, do_ref, w1_ref, w2_ref, b_ref,
                x3_ref, dm3_ref, y3_ref, gain_ref, vin_ref,
                g_ref, gw1_ref, gw2_ref, gb1_ref, gx_ref, vec_ref, yo_ref,
                dqkv_ref, dh_ref, gx_own, v_own, v_all, via_y, via_g,
                outs, pair_in, opp_l, opp_r, near_l, near_r, acc, loc_sem, send_sem, recv_sem):
    hw = heads * hd
    half = 2 * hw
    scale = 1.0 / math.sqrt(hd)
    j = pl.program_id(0)
    m = j - size
    me, right, left, _ = ring(size)
    partner = swap_core(me)
    n, width = h_ref.shape
    rows = outs.shape[1]
    tok = x3_ref.shape[1]
    mlp = w2_ref.shape[0]
    sems = send_sem, recv_sem
    own = 2
    base = 0
    ex_y = Exchange(size, lambda d: y3_ref.at[d], lambda d: yo_ref.at[d], via_y, sems, base)
    base += Exchange.COPIES
    ex_g = Exchange(size, lambda d: gx_own.at[d], lambda d: gx_ref.at[d], via_g, sems, base)
    base += Exchange.COPIES
    local = lambda src, dst, i: pltpu.make_async_copy(src, dst, loc_sem.at[i])
    y_local, gx_local = local(y3_ref.at[me], yo_ref.at[me], 1), local(gx_own.at[me], gx_ref.at[me], 2)

    def numbered(src, dst, i, dev):
        return push(src, dst, send_sem.at[base + i], recv_sem.at[base + i], dev)

    def pair_copy(t):
        return numbered(outs.at[t % own], pair_in.at[t % own], t, partner)

    pairs = size // 2
    lo, hi = pl.ds(0, half), pl.ds(half, rows - half)
    one, two = own + 1, own + 2
    opp_right = lambda: numbered(outs.at[own, lo], opp_l, pairs, right)
    opp_left = lambda: numbered(outs.at[own, hi], opp_r, pairs + 1, left)
    right_hi = lambda: numbered(outs.at[one, hi], near_l.at[hi], pairs + 2, right)
    right_lo = lambda: numbered(outs.at[one, lo], near_l.at[lo], pairs + 3, right)
    left_lo = lambda: numbered(outs.at[two, lo], near_r.at[lo], pairs + 4, left)
    left_hi = lambda: numbered(outs.at[two, hi], near_r.at[hi], pairs + 5, left)

    def v_copy(dev, slot):
        return push(v_own, v_all.at[slot], send_sem.at[base + 2 * size + dev], recv_sem.at[base + 2 * size + slot], dev)

    @pl.when(j == 0)
    def _():
        greet_all(size)
        ex_y.start()
        y_local.start()

    @pl.when(j == 1)
    def _():
        ex_y.forward()

    @pl.when(j < size)
    def _():
        d_mix = mm(dm_ref[...], w_ref[0, 3 * hw:4 * hw], NT).astype(BF16).T
        qkv = qkv_ref[0]
        for h in range(heads):
            q, k, v = (head(qkv, i * heads + h, hd) for i in range(3))
            da = head(d_mix, h, hd)
            s = mm(k, q, TN) * scale
            p = jnp.exp(s - st_ref[0, h:h + 1]) * st_ref[0, heads + h:heads + h + 1]
            dp = mm(v, da, TN).astype(BF16).astype(F32)
            ds = (p * (dp - jnp.sum(p * dp, axis=0, keepdims=True)) * scale).astype(BF16)
            dk = mm(ds, q, NT).astype(BF16).T
            dv = mm(p.astype(BF16), da, NT).astype(BF16).T
            for i, z in enumerate((mm(k, ds, NN).astype(BF16), dk, dv)):
                at = i * hw + h * hd
                dqkv_ref[at:at + hd] = z
        dqkv = dqkv_ref[...]
        part = mm(dqkv, w_ref[0, :3 * hw], TN)

        @pl.when(j == 0)
        def _():
            dh_ref[...] = part

        @pl.when(j > 0)
        def _():
            dh_ref[...] += part

        for t in range(own, pairs):
            @pl.when(j == 2 * t)
            def _():
                pair_copy(t - own).wait_send()

        @pl.when(j == size - 1)
        def _():
            opp_right().wait_send()
            opp_left().wait_send()

        turn = lax.div(j, 2)
        out = outs.at[jnp.where(lax.rem(j, 2) == 0, lax.rem(turn, own), own + lax.rem(turn, pairs - 1))]
        out[:3 * hw] = mm(dqkv, h_ref[...], NN)
        out[3 * hw:4 * hw] = mm(mix_ref[0], dm_ref[...], NN)
        sums = mm(jnp.ones((BIAS_ROWS, n), BF16), dqkv, NT)
        out[4 * hw:] = jnp.concatenate([sums, jnp.zeros((BIAS_ROWS, width - 3 * hw), F32)], axis=1)

        for t in range(pairs):
            @pl.when(j == 2 * t)
            def _():
                pair_copy(t).start()

            @pl.when(j == 2 * t + 1)
            def _():
                pair_copy(t).wait_recv()
                outs[own + t % (pairs - 1)] += pair_in[t % own]

        @pl.when(j == 1)
        def _():
            opp_right().start()
            opp_left().start()

        @pl.when(j == 3)
        def _():
            right_hi().start()

        @pl.when(j == 5)
        def _():
            left_lo().start()

        @pl.when(j == size - 1)
        def _():
            opp_right().wait_recv()
            outs[one, lo] += opp_l[...]
            right_lo().start()
            opp_left().wait_recv()
            outs[two, hi] += opp_r[...]
            left_hi().start()

    @pl.when(m == 0)
    def _():
        v_own[...] = vin_ref[...]

        @pl.loop(0, size)
        def _(dev):
            dh = dh_ref[pl.ds(pl.multiple_of(dev * tok, 8), tok)].astype(BF16).astype(F32)
            xhat, inv = norm_rows(x3_ref[dev].astype(F32))
            gx_own[dev] = (dm3_ref[dev].astype(F32) + norm_rows_pull(xhat, inv, dh, gain_ref[...])).astype(BF16)
            v_own[0:1] += jnp.sum(dh * xhat, axis=0, keepdims=True)
            v_own[1:2] += jnp.sum(dh, axis=0, keepdims=True)

        for r in range(1, size):
            v_copy(lax.rem(me + r, size), me).start()
        ex_g.start()
        gx_local.start()
        v_all[me] = v_own[...]

    @pl.when(m == size - 1)
    def _():
        ex_g.forward()

    @pl.when(m >= 0)
    def _():
        h2 = h2_ref[0]
        do = do_ref[0]
        one_row = (lax.broadcasted_iota(jnp.int32, (BIAS_ROWS, n), 0) == 0).astype(F32).astype(BF16)
        b1 = mm(b_ref[0, :, 3 * hw:3 * hw + mlp], one_row, TN)
        u = (mm(w1_ref[...], h2, NT) + b1).astype(BF16).astype(F32)
        dg = mm(w2_ref[...], do, NT).astype(BF16).astype(F32)
        g, slope = gelu_and_slope(u)
        du = (dg * slope).astype(BF16)
        g1 = mm(du, h2, NN)
        g2 = mm(g.astype(BF16), do, NN)
        gb = mm(jnp.ones((8, n), BF16), du, NT)

        @pl.when(m == 0)
        def _():
            acc[:mlp] = g1
            acc[mlp:] = g2
            gb1_ref[...] = gb

        @pl.when(m > 0)
        def _():
            acc[:mlp] += g1
            acc[mlp:] += g2
            gb1_ref[...] += gb

    @pl.when(m == size - 1)
    def _():
        gw1_ref[...] = acc[:mlp].astype(BF16)
        gw2_ref[...] = acc[mlp:].astype(BF16)
        ring_copies = (right_hi(), right_lo(), left_lo(), left_hi())
        for c in ring_copies:
            c.wait_recv()
        g_ref[...] = (outs[own] + near_l[...] + near_r[...]).astype(BF16)
        for c in ring_copies + (pair_copy(pairs - 2), pair_copy(pairs - 1)):
            c.wait_send()
        for r in range(1, size):
            dev = lax.rem(me + r, size)
            v_copy(dev, dev).wait()
        total = v_all[0]
        for i in range(1, size):
            total += v_all[i]
        vec_ref[...] = total
        ex_y.close()
        ex_g.close()
        gx_local.wait()
        y_local.wait()


def back(h_one, d_mid, wcat, qkv, mix, stats, h2_all, d_out_all, w1t, w_2, x3, y_img, gain, sums, heads, hd):
    size, rows, width = wcat.shape
    n = h_one.shape[0]
    mlp = w_2.shape[0]
    hw = heads * hd
    first = lambda i: block_of_step(jnp.minimum(i, size - 1), size)
    second = lambda i: jnp.maximum(i - size, 0)
    buf = lambda *shape: pltpu.VMEM(shape, F32)
    half_buf = lambda *shape: pltpu.VMEM(shape, BF16)
    bf = lambda *shape: jax.ShapeDtypeStruct(shape, BF16)
    copies = 2 * Exchange.COPIES + 3 * size
    half = 2 * hw
    tokens = x3.shape[1:]
    act3 = whole(*x3.shape)
    return pl.pallas_call(
        functools.partial(back_kernel, heads, hd, size),
        grid=(2 * size,),
        in_specs=[whole(n, width), whole(n, width), block(first, rows, width), block(first, 3 * hw, n), block(first, hw, n),
                  block(first, 2 * heads, n), block(second, n, width), block(second, n, width), whole(mlp, width), whole(mlp, width),
                  pl.BlockSpec((1, BIAS_ROWS, width), lambda i: (lax.axis_index('tp'), rows // BIAS_ROWS - 1, 0)),
                  act3, act3, act3, whole(1, width), whole(*sums.shape)],
        out_specs=[whole(rows, width), whole(mlp, width), whole(mlp, width), whole(8, mlp), ANY, whole(*sums.shape), ANY],
        out_shape=[bf(rows, width), bf(mlp, width), bf(mlp, width), jax.ShapeDtypeStruct((8, mlp), F32), bf(*x3.shape),
                   jax.ShapeDtypeStruct(sums.shape, F32), bf(*x3.shape)],
        scratch_shapes=[half_buf(3 * hw, n), buf(n, width), half_buf(*x3.shape), buf(*sums.shape), buf(size, *sums.shape),
                        half_buf(2, *tokens), half_buf(2, *tokens), buf(size // 2 + 1, rows, width), buf(2, rows, width),
                        buf(half, width), buf(rows - half, width), buf(rows, width), buf(rows, width), buf(2 * mlp, width),
                        dma(3), dma(copies), dma(copies)],
        compiler_params=kernel_params(2),
        name="back",
    )(h_one, d_mid, wcat, qkv, mix, stats, h2_all, d_out_all, w1t, w_2, wcat, x3, d_mid.reshape(x3.shape), y_img.reshape(x3.shape),
      gain, sums)


def finish_kernel(heads, hd, g_ref, gw1_ref, gw2_ref, gb1_ref, gx_ref, y_ref, vec_ref,
                  gq, gk, gv, go, bq, bv, w1_out, b1_out, w2_out, x_out, y_out, *vec_outs):
    hw = heads * hd
    for i, out in enumerate((gq, gk, gv, go)):
        out[...] = g_ref[i * hw:(i + 1) * hw]
    sums = g_ref[4 * hw:].astype(F32)[:1]
    for i, out in ((0, bq), (2, bv)):
        for h in range(heads):
            at = i * hw + h * hd
            out[h:h + 1] = sums[:, at:at + hd].astype(BF16)
    w1_out[...] = gw1_ref[...].T
    b1_out[...] = gb1_ref[0].astype(BF16)
    w2_out[...] = gw2_ref[...]
    x_out[...] = gx_ref[...]
    y_out[...] = y_ref[...]
    for i, out in enumerate(vec_outs):
        out[...] = vec_ref[i].astype(out.dtype)


def finish(g, gw1, gw2, gb1, gx, y, vec, heads, hd):
    width = g.shape[1]
    mlp = gw2.shape[0]
    hw = heads * hd
    bf = lambda *shape: jax.ShapeDtypeStruct(shape, BF16)
    f32_row = jax.ShapeDtypeStruct((width,), F32)
    vm = pl.BlockSpec(memory_space=pltpu.VMEM)
    outs = [bf(hw, width)] * 4 + [bf(heads, hd)] * 2 + [bf(width, mlp), bf(mlp), bf(mlp, width), bf(*gx.shape), bf(*y.shape)]
    outs += [f32_row] * 4 + [bf(width)] * 2
    return pl.pallas_call(
        functools.partial(finish_kernel, heads, hd),
        in_specs=[vm] * 7,
        out_specs=[vm] * len(outs),
        out_shape=outs,
        compiler_params=pltpu.CompilerParams(vmem_limit_bytes=67_043_328),
        name="finish",
    )(g, gw1, gw2, gb1, gx, y, vec)


def solution(mesh):
    act_spec = P('dp', 'tp', None)
    replicated = P()
    head_w = P(None, 'tp', None)
    head_b = P('tp', None)
    grad_head_w = P('dp', 'tp', None)
    grad_head_b = P(('dp', 'tp'), None)
    grad_vec = P('dp')
    in_specs = (act_spec, act_spec, replicated, replicated, head_w, head_b, head_w, head_w, head_b,
                P('tp', None, None), replicated, replicated, replicated, P(None, 'tp'), P('tp'), P('tp', None), replicated)
    out_specs = (act_spec, act_spec, grad_vec, grad_vec, grad_head_w, grad_head_b, grad_head_w, grad_head_w, grad_head_b,
                 P(('dp', 'tp'), None, None), grad_vec, grad_vec, grad_vec, P('dp', 'tp'), P(('dp', 'tp')),
                 P(('dp', 'tp'), None), grad_vec)

    def layer_step(x, d_out, ln1_gain, ln1_bias, w_q, b_q, w_k, w_v, b_v, w_o, b_o, ln2_gain, ln2_bias, w_1, b_1, w_2, b_2):
        width = x.shape[-1]
        heads_loc, hd = w_q.shape[1:]
        hw = heads_loc * hd
        flat = lambda w: w.transpose(1, 2, 0).reshape(hw, width)
        qkv, mixed, stats, h_one, y_img, d_mid, sums, w1t, x_img, wcat, d_out_all, h2_all = front(
            x, (flat(w_q), flat(w_k), flat(w_v), w_o.reshape(hw, width)), (b_q, b_v, b_1),
            (ln1_gain[None], ln1_bias[None], ln2_gain[None], ln2_bias[None]), (b_o, b_2), w_1, w_2, d_out, heads_loc, hd)
        g_all, gw1, gw2, gb1, gx, vec, y_tok = back(
            h_one, d_mid, wcat, qkv, mixed, stats, h2_all, d_out_all, w1t, w_2, x_img, y_img, ln1_gain[None], sums, heads_loc, hd)
        (gq, gk, gv, go, grad_b_q, grad_b_v, grad_w_1, grad_b_1, grad_w_2, grad_x, y_out, g_ln1_gain, g_ln1_bias, g_ln2_gain, g_ln2_bias,
         grad_b_o, grad_b_2) = finish(g_all, gw1, gw2, gb1, gx, y_tok, vec, heads_loc, hd)
        gq, gk, gv = (z.reshape(heads_loc, hd, width).transpose(2, 0, 1) for z in (gq, gk, gv))
        grad_w_o = go.reshape(w_o.shape)
        return (y_out, grad_x, g_ln1_gain, g_ln1_bias, gq, grad_b_q, gk, gv, grad_b_v, grad_w_o,
                grad_b_o, g_ln2_gain, g_ln2_bias, grad_w_1, grad_b_1, grad_w_2, grad_b_2)

    return jax.shard_map(layer_step, mesh=mesh, in_specs=in_specs, out_specs=out_specs, check_vma=False)
```

```python
import functools
import math
import jax
import jax.numpy as jnp
from jax import lax
from jax.experimental import pallas as pl
from jax.experimental.pallas import tpu as pltpu
from jax.sharding import PartitionSpec as P

LN_EPS = 1e-6
F32 = jnp.float32
BF16 = jnp.bfloat16
NN = (((1,), (0,)), ((), ()))
NT = (((1,), (1,)), ((), ()))
TN = (((0,), (0,)), ((), ()))
BIAS_ROWS = 16


def mm(a, b, dims):
    return lax.dot_general(a, b, dims, preferred_element_type=F32)


def push(src, dst, ssem, rsem, dev):
    return pltpu.make_async_remote_copy(src_ref=src, dst_ref=dst, send_sem=ssem, recv_sem=rsem,
                                        device_id={'tp': dev}, device_id_type=pl.DeviceIdType.MESH)


def greet_all(size):
    me = lax.axis_index('tp')
    barrier = pltpu.get_barrier_semaphore()
    for r in range(1, size):
        pl.semaphore_signal(barrier, inc=1, device_id={'tp': lax.rem(me + r, size)}, device_id_type=pl.DeviceIdType.MESH)
    pl.semaphore_wait(barrier, size - 1)


def swap_core(dev):
    return dev + 1 - 2 * lax.rem(dev, 2)


def ring(size):
    me = lax.axis_index('tp')
    return me, lax.rem(me + 2, size), lax.rem(me + size - 2, size), lax.rem(me + size // 2, size)


class Gather:
    COPIES = 14

    def __init__(self, size, src, dst, sems, off):
        me, right, left, opp = ring(size)
        partner = swap_core(me)
        plan = [(me, 0, right), (me, 1, right), (left, 0, right), (me, 1, left), (me, 0, left), (right, 1, left)]
        plan += [(owner, half, partner) for owner in (me, left, right, opp) for half in range(2)]

        def make(i):
            owner, half, dev = plan[i]
            out = dst(owner, half)
            return push(src(half) if owner is me else out, out, sems[0].at[off + i], sems[1].at[off + i], dev)

        self.copy = make

    def start(self):
        for i in (0, 3, 1, 4, 6, 7):
            self.copy(i).start()

    def forward(self):
        for got, sends in ((0, (2, 8)), (3, (5, 11))):
            self.copy(got).wait_recv()
            for i in sends:
                self.copy(i).start()

    def relay(self, *pairs):
        for got, i in pairs:
            self.copy(got).wait_recv()
            self.copy(i).start()

    def near(self):
        self.relay((1, 9), (4, 10))

    def far(self):
        self.relay((2, 12), (5, 13))

    def received(self, *which):
        for i in which:
            self.copy(i).wait_recv()

    def sent(self):
        for i in range(self.COPIES):
            self.copy(i).wait_send()

    def follow(self, step, *ahead):
        def at(k, *calls):
            @pl.when(step == k)
            def _():
                for call in calls:
                    call()

        at(1, lambda: self.received(6, 7))
        at(2, *ahead, lambda: self.relay((1, 9)))
        at(3, lambda: self.relay((4, 10)))
        at(4, lambda: self.received(8, 9))
        at(5, lambda: self.received(10, 11))
        at(6, self.far)
        at(7, lambda: self.received(12, 13))


class Exchange:
    COPIES = 9

    def __init__(self, size, src, dst, via, sems, off):
        me, right, left, opp = ring(size)
        plan = [(src(opp), via.at[0], left), (src(swap_core(opp)), via.at[1], right)]
        plan += [(src(dev), dst(me), dev) for side in (right, left) for dev in (side, swap_core(side))]
        plan += [(src(swap_core(me)), dst(me), swap_core(me)), (via.at[0], dst(right), left), (via.at[1], dst(left), swap_core(right))]
        self.copy = lambda i: push(*plan[i][:2], sems[0].at[off + i], sems[1].at[off + i], plan[i][2])

    def start(self):
        for i in range(7):
            self.copy(i).start()

    def forward(self):
        for got, i in ((0, 7), (1, 8)):
            self.copy(got).wait_recv()
            self.copy(i).start()

    def close(self):
        for i in range(2, self.COPIES):
            self.copy(i).wait_recv()
        for i in range(self.COPIES):
            self.copy(i).wait_send()


def pair_rows(ref, c):
    return jnp.concatenate([ref[2 * c].astype(F32), ref[2 * c + 1].astype(F32)])


def pair_chunks(size, tok, body):
    pl.loop(0, size // 2)(lambda c: body(c, pl.ds(pl.multiple_of(c * 2 * tok, 16), 2 * tok)))


def cut(rows):
    half = rows // 2 // 16 * 16
    return pl.ds(0, half), pl.ds(half, rows - half)


def head(z, i, hd):
    return z[i * hd:(i + 1) * hd]


def norm_rows(z):
    centered = z - jnp.mean(z, axis=-1, keepdims=True)
    inv = lax.rsqrt(jnp.mean(centered * centered, axis=-1, keepdims=True) + LN_EPS)
    return centered * inv, inv


def norm_rows_pull(xhat, inv, dh, gain):
    dxh = dh * gain
    return inv * (dxh - jnp.mean(dxh, axis=-1, keepdims=True) - xhat * jnp.mean(dxh * xhat, axis=-1, keepdims=True))


def arrival(i, size):
    me = lax.axis_index('tp')
    partner = me + 1 - 2 * lax.rem(me, 2)
    hop = jnp.where(i < 2, 0, jnp.where(i >= 6, size // 2, jnp.where(lax.rem(i, 2) == 0, size - 2, 2)))
    base = jnp.where((i == 1) | (i == 4) | (i == 5) | (i == 7), partner, me)
    return lax.rem(base + hop, size)


def gelu_and_slope(u):
    c = math.sqrt(2.0 / math.pi)
    u2 = u * u
    t = jnp.tanh(c * (u + 0.044715 * (u2 * u)))
    half = 0.5 * (1.0 + t)
    slope = half + 0.5 * u * (1.0 - t * t) * (c * (1.0 + (3.0 * 0.044715) * u2))
    return u * half, slope


def front_kernel(heads, hd, size, x_ref, wq_ref, wk_ref, wv_ref, wo_ref, bq_ref, bv_ref, b1_ref,
                 g1_ref, c1_ref, g2_ref, c2_ref, bo_ref, b2_ref, w1_ref, w2_ref, do_ref,
                 qkv_ref, mix_ref, st_ref, h1_out, y_out, dm_out, sums_ref, w1t_out, xi_ref, wa_ref, doa_ref, h2a_ref,
                 h1_ref, y_ref, dm_ref, w1t_ref, wl_ref, w_all, w1_all, w2_all, x_all, via, acc_ref, dacc, own_do, d_img, xm_ref, h2_ref, loc_sem, out_sem, send_sem, recv_sem):
    hw = heads * hd
    scale = 1.0 / math.sqrt(hd)
    step = pl.program_id(0)
    k = step - size
    mlp = w2_ref.shape[0]
    me = lax.axis_index('tp')
    imgs, tok, width = x_ref.shape
    n = h1_ref.shape[0]
    g1, c1, g2, c2 = g1_ref[...], c1_ref[...], g2_ref[...], c2_ref[...]
    bo, b2 = (r[...].astype(F32).reshape(1, width) for r in (bo_ref, b2_ref))
    rows = wl_ref.shape[0]
    sems = send_sem, recv_sem
    images = pl.ds(0, imgs // 2), pl.ds(imgs // 2, imgs // 2)
    mine = lambda dev: pl.ds(pl.multiple_of(dev * tok, 8), tok)
    gw = Gather(size, lambda h: wl_ref.at[cut(rows)[h]], lambda d, h: w_all.at[d, cut(rows)[h]], sems, 0)
    gw1 = Gather(size, lambda h: w1_ref.at[cut(width)[h]], lambda d, h: w1_all.at[d, cut(width)[h]], sems, Gather.COPIES)
    gdo = Gather(size, lambda h: do_ref.at[images[h]], lambda d, h: doa_ref.at[images[h], mine(d)], sems, 2 * Gather.COPIES)
    gw2 = Gather(size, lambda h: w2_ref.at[cut(mlp)[h]], lambda d, h: w2_all.at[d, cut(mlp)[h]], sems, 3 * Gather.COPIES)
    gh2 = Gather(size, lambda h: h2_ref.at[cut(n)[h]], lambda d, h: h2a_ref.at[d, cut(n)[h]], sems, 4 * Gather.COPIES)
    ex = Exchange(size, lambda d: x_ref.at[d], lambda d: x_all.at[d], via, sems, 5 * Gather.COPIES)
    local = lambda src, dst, i: pltpu.make_async_copy(src, dst, loc_sem.at[i])
    in_x, in_do = local(x_ref.at[me], x_all.at[me], 0), local(do_ref, own_do, 1)
    out_w, out_h2 = local(wl_ref, wa_ref.at[me], 2), local(h2_ref, h2a_ref.at[me], 3)
    in_img = local(doa_ref.at[me], d_img, 6)
    out_h1, out_w1t, out_y, out_dm = local(h1_ref, h1_out, 7), local(w1t_ref, w1t_out, 8), local(y_ref, y_out, 9), local(dm_ref, dm_out, 10)
    out_x, out_do = local(x_all, xi_ref, 4), local(own_do, doa_ref.at[:, mine(me)], 5)

    def out_block(i):
        dev = arrival(i, size)
        return pltpu.make_async_copy(w_all.at[dev], wa_ref.at[dev], out_sem.at[i])

    @pl.when(step == 0)
    def _():
        in_x.start()
        in_do.start()
        greet_all(size)
        ex.start()
        for i, part in enumerate((wq_ref, wk_ref, wv_ref, wo_ref)):
            wl_ref[i * hw:(i + 1) * hw] = part[...]
        zeros = jnp.zeros((1, hw), F32)
        pieces = [r[h:h + 1].astype(F32) for r in (bq_ref, bv_ref) for h in range(heads)]
        line = jnp.concatenate(pieces[:heads] + [zeros] + pieces[heads:] + [b1_ref[...].astype(F32).reshape(1, mlp)]
                               + [zeros] * ((width - 3 * hw - mlp) // hw), axis=1)
        wl_ref[4 * hw:] = jnp.where(lax.broadcasted_iota(jnp.int32, (BIAS_ROWS, width), 0) == 0, line, 0.0).astype(BF16)
        ex.forward()
        gw.start()
        out_w.start()
        w_all[me] = wl_ref[...]
        in_x.wait()
        ex.close()
        out_x.start()

        def body(c, rows):
            xhat, _ = norm_rows(pair_rows(x_all, c))
            h1_ref[rows] = (xhat * g1 + c1).astype(BF16)

        pair_chunks(size, tok, body)
        in_do.wait()
        out_do.start()

    gw.follow(step, gw.forward, gdo.start)

    @pl.when((step > 0) & (k < 0))
    def _():
        out_block(step).start()

    @pl.when(k < 0)
    def _():
        w = w_all.at[arrival(step, size)]
        bias = mm(w[4 * hw:, :3 * hw], jnp.ones((BIAS_ROWS, n), BF16), TN)
        qkv = (mm(w[:3 * hw], h1_ref[...], NT) + bias).astype(BF16)
        qkv_ref[0] = qkv
        for h in range(heads):
            q, key, v = (head(qkv, i * heads + h, hd) for i in range(3))
            s = mm(key, q, TN) * scale
            top = jnp.max(s, axis=0, keepdims=True)
            e = jnp.exp(s - top)
            inv = 1.0 / jnp.sum(e, axis=0, keepdims=True)
            st_ref[0, h:h + 1] = top
            st_ref[0, heads + h:heads + h + 1] = inv
            mix_ref[0, h * hd:(h + 1) * hd] = mm(v, (e * inv).astype(BF16), NN).astype(BF16)
        out = mm(mix_ref[0], w[3 * hw:4 * hw], TN)

        @pl.when(step == 0)
        def _():
            acc_ref[...] = out

        @pl.when(step > 0)
        def _():
            acc_ref[...] += out

    @pl.when(k == -1)
    def _():
        gdo.forward()
        gw1.start()

        def body(c, rows):
            mid = (pair_rows(x_all, c) + acc_ref[rows] + bo).astype(BF16)
            xm_ref[rows] = mid
            xhat, _ = norm_rows(mid.astype(F32))
            h2_ref[rows] = (xhat * g2 + c2).astype(BF16)

        pair_chunks(size, tok, body)

    @pl.when(k == 0)
    def _():
        out_h2.start()
        w1_all[me] = w1_ref[...]
        w2_all[me] = w2_ref[...]
        w1t_ref[...] = w1_ref[...].T
        gdo.near()
        gdo.far()
        gw1.forward()
        gw2.start()
        gdo.received(*range(6, Gather.COPIES))
        out_do.wait()
        in_img.start()
        in_img.wait()

    gw1.follow(k, out_h1.start, out_w1t.start)
    gw2.follow(k, gw2.forward, gh2.start)

    @pl.when(k >= 0)
    def _():
        dev = arrival(k, size)
        w1, w2 = w1_all[dev], w2_all[dev]
        b1 = w_all[dev, 4 * hw:4 * hw + 1, 3 * hw:3 * hw + mlp].astype(F32)
        u = (mm(h2_ref[...], w1, NN) + b1).astype(BF16).astype(F32)
        dg = mm(d_img[...], w2, NT).astype(BF16).astype(F32)
        g, slope = gelu_and_slope(u)
        ypart = mm(g.astype(BF16), w2, NN)
        dpart = mm((dg * slope).astype(BF16), w1, NT)

        @pl.when(k == 0)
        def _():
            acc_ref[...] = ypart
            dacc[...] = dpart

        @pl.when(k > 0)
        def _():
            acc_ref[...] += ypart
            dacc[...] += dpart

    @pl.when(k == size - 1)
    def _():
        sums_ref[...] = jnp.zeros_like(sums_ref)

        def body(c, part):
            mid = xm_ref[part].astype(F32)
            y_ref[part] = (mid + acc_ref[part] + b2).astype(BF16)
            xhat, inv = norm_rows(mid)
            dh = dacc[part].astype(BF16).astype(F32)
            do = d_img[part].astype(F32)
            dm = (do + norm_rows_pull(xhat, inv, dh, g2)).astype(BF16)
            dm_ref[part] = dm
            for i, v in enumerate((dh * xhat, dh, dm.astype(F32), do)):
                sums_ref[2 + i:3 + i] += jnp.sum(v, axis=0, keepdims=True)

        gh2.forward()
        pair_chunks(size, tok, body)
        gh2.near()
        out_y.start()
        out_dm.start()
        gh2.far()
        gh2.received(*range(6, Gather.COPIES))
        for g in (gw, gw1, gdo, gw2, gh2):
            g.sent()
        for c in (out_x, out_w, out_h2, out_h1, out_w1t, out_y, out_dm):
            c.wait()
        for i in range(1, size):
            out_block(i).wait()


def whole(*shape):
    return pl.BlockSpec(shape, lambda i: (0,) * len(shape), pipeline_mode=pl.Buffered(1))


def block(index, *shape):
    return pl.BlockSpec((1,) + shape, lambda i: (index(i),) + (0,) * len(shape))


def dma(k):
    return pltpu.SemaphoreType.DMA((k,))


def kernel_params(collective_id):
    return pltpu.CompilerParams(dimension_semantics=("arbitrary",), vmem_limit_bytes=67_043_328,
                                collective_id=collective_id, has_side_effects=True)


ANY = pl.BlockSpec(memory_space=pl.ANY)


def front(x, weights, biases, gains, sums_bias, w_1, w_2, d_out, heads, hd):
    imgs, tok, width = x.shape
    size = imgs
    n = size * tok
    hw = heads * hd
    mlp = w_2.shape[0]
    rows = 4 * hw + BIAS_ROWS
    order = lambda i: arrival(jnp.minimum(i, size - 1), size)
    bf = lambda *shape: jax.ShapeDtypeStruct(shape, BF16)
    buf = lambda *shape: pltpu.VMEM(shape, BF16)
    copies = 5 * Gather.COPIES + Exchange.COPIES
    return pl.pallas_call(
        functools.partial(front_kernel, heads, hd, size),
        grid=(2 * size,),
        in_specs=[ANY] + [whole(*z.shape) for z in weights + biases + gains + sums_bias] + [ whole(width, mlp), whole(mlp, width), ANY],
        out_specs=[block(order, 3 * hw, n), block(order, hw, n), block(order, 2 * heads, n), ANY, ANY, ANY, whole(8, width)]
                  + [ANY] * 5,
        out_shape=[bf(size, 3 * hw, n), bf(size, hw, n), jax.ShapeDtypeStruct((size, 2 * heads, n), F32), bf(n, width), bf(n, width),
                   bf(n, width), jax.ShapeDtypeStruct((8, width), F32), bf(mlp, width),
                   bf(size, tok, width), bf(size, rows, width), bf(imgs, n, width), bf(size, n, width)],
        scratch_shapes=[buf(n, width), buf(n, width), buf(n, width), buf(mlp, width), buf(rows, width), buf(size, rows, width), buf(size, width, mlp), buf(size, mlp, width), buf(size, tok, width), buf(2, tok, width),
                        pltpu.VMEM((n, width), F32), pltpu.VMEM((n, width), F32), buf(*d_out.shape), buf(n, width), buf(n, width),
                        buf(n, width), dma(11), dma(size), dma(copies), dma(copies)],
        compiler_params=kernel_params(1),
        name="front",
    )(x, *weights, *biases, *gains, *sums_bias, w_1, w_2, d_out)


def block_of_step(j, size):
    me = lax.axis_index('tp')
    chips = size // 2
    off = jnp.where(j < 2, 2, jnp.where(j < 4, 1, jnp.where(j < 6, 3, 0)))
    chip = lax.rem(lax.div(me, 2) + off, chips)
    core = lax.rem(me, 2)
    side = jnp.where(lax.rem(j, 2) == 0, 1 - core, core)
    return 2 * chip + side


def back_kernel(heads, hd, size, h_ref, dm_ref, w_ref, qkv_ref, mix_ref, st_ref, h2_ref, do_ref, w1_in, w2_in, b_ref,
                x3_in, dm3_in, y3_ref, gain_ref, vin_ref,
                g_out, gw1_out, gw2_out, gb1_ref, gx_ref, vec_ref, yo_ref,
                w1_ref, w2_ref, x3_ref, dm3_ref, g_ref, gw1_ref, gw2_ref,
                dqkv_ref, dh_ref, gx_own, v_own, v_all, via_y, via_g,
                outs, pair_in, opp_l, opp_r, near_l, near_r, acc, loc_sem, send_sem, recv_sem):
    hw = heads * hd
    half = 2 * hw
    scale = 1.0 / math.sqrt(hd)
    j = pl.program_id(0)
    m = j - size
    me, right, left, _ = ring(size)
    partner = swap_core(me)
    n, width = h_ref.shape
    rows = outs.shape[1]
    tok = x3_ref.shape[1]
    mlp = w2_ref.shape[0]
    sems = send_sem, recv_sem
    own = 2
    base = 0
    ex_y = Exchange(size, lambda d: y3_ref.at[d], lambda d: yo_ref.at[d], via_y, sems, base)
    base += Exchange.COPIES
    ex_g = Exchange(size, lambda d: gx_own.at[d], lambda d: gx_ref.at[d], via_g, sems, base)
    base += Exchange.COPIES
    local = lambda src, dst, i: pltpu.make_async_copy(src, dst, loc_sem.at[i])
    y_local, gx_local = local(y3_ref.at[me], yo_ref.at[me], 1), local(gx_own.at[me], gx_ref.at[me], 2)
    late = [local(src, dst, 3 + i) for i, (src, dst) in enumerate(((x3_in, x3_ref), (dm3_in, dm3_ref), (w1_in, w1_ref), (w2_in, w2_ref)))]
    outward = [local(src, dst, 7 + i) for i, (src, dst) in enumerate(((gw1_ref, gw1_out), (gw2_ref, gw2_out), (g_ref, g_out)))]

    def numbered(src, dst, i, dev):
        return push(src, dst, send_sem.at[base + i], recv_sem.at[base + i], dev)

    def pair_copy(t):
        return numbered(outs.at[t % own], pair_in.at[t % own], t, partner)

    pairs = size // 2
    lo, hi = pl.ds(0, half), pl.ds(half, rows - half)
    one, two = own + 1, own + 2
    opp_right = lambda: numbered(outs.at[own, lo], opp_l, pairs, right)
    opp_left = lambda: numbered(outs.at[own, hi], opp_r, pairs + 1, left)
    right_hi = lambda: numbered(outs.at[one, hi], near_l.at[hi], pairs + 2, right)
    right_lo = lambda: numbered(outs.at[one, lo], near_l.at[lo], pairs + 3, right)
    left_lo = lambda: numbered(outs.at[two, lo], near_r.at[lo], pairs + 4, left)
    left_hi = lambda: numbered(outs.at[two, hi], near_r.at[hi], pairs + 5, left)

    def v_copy(dev, slot):
        return push(v_own, v_all.at[slot], send_sem.at[base + 2 * size + dev], recv_sem.at[base + 2 * size + slot], dev)

    @pl.when(j == 0)
    def _():
        greet_all(size)
        ex_y.start()
        y_local.start()
        for c in late:
            c.start()

    @pl.when(j == 1)
    def _():
        ex_y.forward()

    @pl.when(j < size)
    def _():
        d_mix = mm(dm_ref[...], w_ref[0, 3 * hw:4 * hw], NT).astype(BF16).T
        qkv = qkv_ref[0]
        for h in range(heads):
            q, k, v = (head(qkv, i * heads + h, hd) for i in range(3))
            da = head(d_mix, h, hd)
            s = mm(k, q, TN) * scale
            p = jnp.exp(s - st_ref[0, h:h + 1]) * st_ref[0, heads + h:heads + h + 1]
            dp = mm(v, da, TN).astype(BF16).astype(F32)
            ds = (p * (dp - jnp.sum(p * dp, axis=0, keepdims=True)) * scale).astype(BF16)
            dk = mm(ds, q, NT).astype(BF16).T
            dv = mm(p.astype(BF16), da, NT).astype(BF16).T
            for i, z in enumerate((mm(k, ds, NN).astype(BF16), dk, dv)):
                at = i * hw + h * hd
                dqkv_ref[at:at + hd] = z
        dqkv = dqkv_ref[...]
        part = mm(dqkv, w_ref[0, :3 * hw], TN)

        @pl.when(j == 0)
        def _():
            dh_ref[...] = part

        @pl.when(j > 0)
        def _():
            dh_ref[...] += part

        for t in range(own, pairs):
            @pl.when(j == 2 * t)
            def _():
                pair_copy(t - own).wait_send()

        @pl.when(j == size - 1)
        def _():
            opp_right().wait_send()
            opp_left().wait_send()

        turn = lax.div(j, 2)
        out = outs.at[jnp.where(lax.rem(j, 2) == 0, lax.rem(turn, own), own + lax.rem(turn, pairs - 1))]
        out[:3 * hw] = mm(dqkv, h_ref[...], NN)
        out[3 * hw:4 * hw] = mm(mix_ref[0], dm_ref[...], NN)
        sums = mm(jnp.ones((BIAS_ROWS, n), BF16), dqkv, NT)
        out[4 * hw:] = jnp.concatenate([sums, jnp.zeros((BIAS_ROWS, width - 3 * hw), F32)], axis=1)

        for t in range(pairs):
            @pl.when(j == 2 * t)
            def _():
                pair_copy(t).start()

            @pl.when(j == 2 * t + 1)
            def _():
                pair_copy(t).wait_recv()
                outs[own + t % (pairs - 1)] += pair_in[t % own]

        @pl.when(j == 1)
        def _():
            opp_right().start()
            opp_left().start()

        @pl.when(j == 3)
        def _():
            right_hi().start()

        @pl.when(j == 5)
        def _():
            left_lo().start()

        @pl.when(j == size - 1)
        def _():
            opp_right().wait_recv()
            outs[one, lo] += opp_l[...]
            right_lo().start()
            opp_left().wait_recv()
            outs[two, hi] += opp_r[...]
            left_hi().start()

    @pl.when(m == 0)
    def _():
        v_own[...] = vin_ref[...]
        for c in late:
            c.wait()

        @pl.loop(0, size)
        def _(dev):
            dh = dh_ref[pl.ds(pl.multiple_of(dev * tok, 8), tok)].astype(BF16).astype(F32)
            xhat, inv = norm_rows(x3_ref[dev].astype(F32))
            gx_own[dev] = (dm3_ref[dev].astype(F32) + norm_rows_pull(xhat, inv, dh, gain_ref[...])).astype(BF16)
            v_own[0:1] += jnp.sum(dh * xhat, axis=0, keepdims=True)
            v_own[1:2] += jnp.sum(dh, axis=0, keepdims=True)

        for r in range(1, size):
            v_copy(lax.rem(me + r, size), me).start()
        ex_g.start()
        gx_local.start()
        v_all[me] = v_own[...]

    @pl.when(m == size - 1)
    def _():
        ex_g.forward()

    @pl.when(m >= 0)
    def _():
        h2 = h2_ref[0]
        do = do_ref[0]
        one_row = (lax.broadcasted_iota(jnp.int32, (BIAS_ROWS, n), 0) == 0).astype(F32).astype(BF16)
        b1 = mm(b_ref[0, :, 3 * hw:3 * hw + mlp], one_row, TN)
        u = (mm(w1_ref[...], h2, NT) + b1).astype(BF16).astype(F32)
        dg = mm(w2_ref[...], do, NT).astype(BF16).astype(F32)
        g, slope = gelu_and_slope(u)
        du = (dg * slope).astype(BF16)
        g1 = mm(du, h2, NN)
        g2 = mm(g.astype(BF16), do, NN)
        gb = mm(jnp.ones((8, n), BF16), du, NT)

        @pl.when(m == 0)
        def _():
            acc[:mlp] = g1
            acc[mlp:] = g2
            gb1_ref[...] = gb

        @pl.when(m > 0)
        def _():
            acc[:mlp] += g1
            acc[mlp:] += g2
            gb1_ref[...] += gb

    @pl.when(m == size - 1)
    def _():
        gw1_ref[...] = acc[:mlp].astype(BF16)
        gw2_ref[...] = acc[mlp:].astype(BF16)
        ring_copies = (right_hi(), right_lo(), left_lo(), left_hi())
        for c in ring_copies:
            c.wait_recv()
        outward[0].start()
        outward[1].start()
        g_ref[...] = (outs[own] + near_l[...] + near_r[...]).astype(BF16)
        for c in ring_copies + (pair_copy(pairs - 2), pair_copy(pairs - 1)):
            c.wait_send()
        for r in range(1, size):
            dev = lax.rem(me + r, size)
            v_copy(dev, dev).wait()
        total = v_all[0]
        for i in range(1, size):
            total += v_all[i]
        vec_ref[...] = total
        outward[2].start()
        ex_y.close()
        ex_g.close()
        gx_local.wait()
        y_local.wait()
        for c in outward:
            c.wait()


def back(h_one, d_mid, wcat, qkv, mix, stats, h2_all, d_out_all, w1t, w_2, x3, y_img, gain, sums, heads, hd):
    size, rows, width = wcat.shape
    n = h_one.shape[0]
    mlp = w_2.shape[0]
    hw = heads * hd
    first = lambda i: block_of_step(jnp.minimum(i, size - 1), size)
    second = lambda i: jnp.maximum(i - size, 0)
    buf = lambda *shape: pltpu.VMEM(shape, F32)
    half_buf = lambda *shape: pltpu.VMEM(shape, BF16)
    bf = lambda *shape: jax.ShapeDtypeStruct(shape, BF16)
    copies = 2 * Exchange.COPIES + 3 * size
    half = 2 * hw
    tokens = x3.shape[1:]
    act3 = whole(*x3.shape)
    return pl.pallas_call(
        functools.partial(back_kernel, heads, hd, size),
        grid=(2 * size,),
        in_specs=[whole(n, width), whole(n, width), block(first, rows, width), block(first, 3 * hw, n), block(first, hw, n),
                  block(first, 2 * heads, n), block(second, n, width), block(second, n, width), ANY, ANY,
                  pl.BlockSpec((1, BIAS_ROWS, width), lambda i: (lax.axis_index('tp'), rows // BIAS_ROWS - 1, 0)),
                  ANY, ANY, act3, whole(1, width), whole(*sums.shape)],
        out_specs=[ANY, ANY, ANY, whole(8, mlp), ANY, whole(*sums.shape), ANY],
        out_shape=[bf(rows, width), bf(mlp, width), bf(mlp, width), jax.ShapeDtypeStruct((8, mlp), F32), bf(*x3.shape),
                   jax.ShapeDtypeStruct(sums.shape, F32), bf(*x3.shape)],
        scratch_shapes=[half_buf(mlp, width), half_buf(mlp, width), half_buf(*x3.shape), half_buf(*x3.shape), half_buf(rows, width),
                        half_buf(mlp, width), half_buf(mlp, width), half_buf(3 * hw, n), buf(n, width), half_buf(*x3.shape), buf(*sums.shape), buf(size, *sums.shape),
                        half_buf(2, *tokens), half_buf(2, *tokens), buf(size // 2 + 1, rows, width), buf(2, rows, width),
                        buf(half, width), buf(rows - half, width), buf(rows, width), buf(rows, width), buf(2 * mlp, width),
                        dma(10), dma(copies), dma(copies)],
        compiler_params=kernel_params(2),
        name="back",
    )(h_one, d_mid, wcat, qkv, mix, stats, h2_all, d_out_all, w1t, w_2, wcat, x3, d_mid.reshape(x3.shape), y_img.reshape(x3.shape),
      gain, sums)


def finish_kernel(heads, hd, g_ref, gw1_ref, gw2_ref, gb1_ref, gx_ref, y_ref, vec_ref,
                  gq, gk, gv, go, bq, bv, w1_out, b1_out, w2_out, x_out, y_out, *vec_outs):
    hw = heads * hd
    for i, out in enumerate((gq, gk, gv, go)):
        out[...] = g_ref[i * hw:(i + 1) * hw]
    sums = g_ref[4 * hw:].astype(F32)[:1]
    for i, out in ((0, bq), (2, bv)):
        for h in range(heads):
            at = i * hw + h * hd
            out[h:h + 1] = sums[:, at:at + hd].astype(BF16)
    w1_out[...] = gw1_ref[...].T
    b1_out[...] = gb1_ref[0].astype(BF16)
    w2_out[...] = gw2_ref[...]
    x_out[...] = gx_ref[...]
    y_out[...] = y_ref[...]
    for i, out in enumerate(vec_outs):
        out[...] = vec_ref[i].astype(out.dtype)


def finish(g, gw1, gw2, gb1, gx, y, vec, heads, hd):
    width = g.shape[1]
    mlp = gw2.shape[0]
    hw = heads * hd
    bf = lambda *shape: jax.ShapeDtypeStruct(shape, BF16)
    f32_row = jax.ShapeDtypeStruct((width,), F32)
    vm = pl.BlockSpec(memory_space=pltpu.VMEM)
    outs = [bf(hw, width)] * 4 + [bf(heads, hd)] * 2 + [bf(width, mlp), bf(mlp), bf(mlp, width), bf(*gx.shape), bf(*y.shape)]
    outs += [f32_row] * 4 + [bf(width)] * 2
    return pl.pallas_call(
        functools.partial(finish_kernel, heads, hd),
        in_specs=[vm] * 7,
        out_specs=[vm] * len(outs),
        out_shape=outs,
        compiler_params=pltpu.CompilerParams(vmem_limit_bytes=67_043_328),
        name="finish",
    )(g, gw1, gw2, gb1, gx, y, vec)


def solution(mesh):
    act_spec = P('dp', 'tp', None)
    replicated = P()
    head_w = P(None, 'tp', None)
    head_b = P('tp', None)
    grad_head_w = P('dp', 'tp', None)
    grad_head_b = P(('dp', 'tp'), None)
    grad_vec = P('dp')
    in_specs = (act_spec, act_spec, replicated, replicated, head_w, head_b, head_w, head_w, head_b,
                P('tp', None, None), replicated, replicated, replicated, P(None, 'tp'), P('tp'), P('tp', None), replicated)
    out_specs = (act_spec, act_spec, grad_vec, grad_vec, grad_head_w, grad_head_b, grad_head_w, grad_head_w, grad_head_b,
                 P(('dp', 'tp'), None, None), grad_vec, grad_vec, grad_vec, P('dp', 'tp'), P(('dp', 'tp')),
                 P(('dp', 'tp'), None), grad_vec)

    def layer_step(x, d_out, ln1_gain, ln1_bias, w_q, b_q, w_k, w_v, b_v, w_o, b_o, ln2_gain, ln2_bias, w_1, b_1, w_2, b_2):
        width = x.shape[-1]
        heads_loc, hd = w_q.shape[1:]
        hw = heads_loc * hd
        flat = lambda w: w.transpose(1, 2, 0).reshape(hw, width)
        qkv, mixed, stats, h_one, y_img, d_mid, sums, w1t, x_img, wcat, d_out_all, h2_all = front(
            x, (flat(w_q), flat(w_k), flat(w_v), w_o.reshape(hw, width)), (b_q, b_v, b_1),
            (ln1_gain[None], ln1_bias[None], ln2_gain[None], ln2_bias[None]), (b_o, b_2), w_1, w_2, d_out, heads_loc, hd)
        g_all, gw1, gw2, gb1, gx, vec, y_tok = back(
            h_one, d_mid, wcat, qkv, mixed, stats, h2_all, d_out_all, w1t, w_2, x_img, y_img, ln1_gain[None], sums, heads_loc, hd)
        (gq, gk, gv, go, grad_b_q, grad_b_v, grad_w_1, grad_b_1, grad_w_2, grad_x, y_out, g_ln1_gain, g_ln1_bias, g_ln2_gain, g_ln2_bias,
         grad_b_o, grad_b_2) = finish(g_all, gw1, gw2, gb1, gx, y_tok, vec, heads_loc, hd)
        gq, gk, gv = (z.reshape(heads_loc, hd, width).transpose(2, 0, 1) for z in (gq, gk, gv))
        grad_w_o = go.reshape(w_o.shape)
        return (y_out, grad_x, g_ln1_gain, g_ln1_bias, gq, grad_b_q, gk, gv, grad_b_v, grad_w_o,
                grad_b_o, g_ln2_gain, g_ln2_bias, grad_w_1, grad_b_1, grad_w_2, grad_b_2)

    return jax.shard_map(layer_step, mesh=mesh, in_specs=in_specs, out_specs=out_specs, check_vma=False)
```

```python
import functools
import math
import jax
import jax.numpy as jnp
from jax import lax
from jax.experimental import pallas as pl
from jax.experimental.pallas import tpu as pltpu
from jax.sharding import PartitionSpec as P

LN_EPS = 1e-6
F32 = jnp.float32
BF16 = jnp.bfloat16
NN = (((1,), (0,)), ((), ()))
NT = (((1,), (1,)), ((), ()))
TN = (((0,), (0,)), ((), ()))
BIAS_ROWS = 16


def mm(a, b, dims):
    return lax.dot_general(a, b, dims, preferred_element_type=F32)


def push(src, dst, ssem, rsem, dev):
    return pltpu.make_async_remote_copy(src_ref=src, dst_ref=dst, send_sem=ssem, recv_sem=rsem,
                                        device_id={'tp': dev}, device_id_type=pl.DeviceIdType.MESH)


def greet_all(size):
    me = lax.axis_index('tp')
    barrier = pltpu.get_barrier_semaphore()
    for r in range(1, size):
        pl.semaphore_signal(barrier, inc=1, device_id={'tp': lax.rem(me + r, size)}, device_id_type=pl.DeviceIdType.MESH)
    pl.semaphore_wait(barrier, size - 1)


def swap_core(dev):
    return dev + 1 - 2 * lax.rem(dev, 2)


def ring(size):
    me = lax.axis_index('tp')
    return me, lax.rem(me + 2, size), lax.rem(me + size - 2, size), lax.rem(me + size // 2, size)


class Gather:
    COPIES = 14

    def __init__(self, size, src, dst, sems, off):
        me, right, left, opp = ring(size)
        partner = swap_core(me)
        plan = [(me, 0, right), (me, 1, right), (left, 0, right), (me, 1, left), (me, 0, left), (right, 1, left)]
        plan += [(owner, half, partner) for owner in (me, left, right, opp) for half in range(2)]

        def make(i):
            owner, half, dev = plan[i]
            out = dst(owner, half)
            return push(src(half) if owner is me else out, out, sems[0].at[off + i], sems[1].at[off + i], dev)

        self.copy = make

    def start(self):
        for i in (0, 3, 1, 4, 6, 7):
            self.copy(i).start()

    def forward(self):
        for got, sends in ((0, (2, 8)), (3, (5, 11))):
            self.copy(got).wait_recv()
            for i in sends:
                self.copy(i).start()

    def relay(self, *pairs):
        for got, i in pairs:
            self.copy(got).wait_recv()
            self.copy(i).start()

    def near(self):
        self.relay((1, 9), (4, 10))

    def far(self):
        self.relay((2, 12), (5, 13))

    def received(self, *which):
        for i in which:
            self.copy(i).wait_recv()

    def sent(self):
        for i in range(self.COPIES):
            self.copy(i).wait_send()

    def follow(self, step, *ahead):
        def at(k, *calls):
            @pl.when(step == k)
            def _():
                for call in calls:
                    call()

        at(1, lambda: self.received(6, 7))
        at(2, *ahead, lambda: self.relay((1, 9)))
        at(3, lambda: self.relay((4, 10)))
        at(4, lambda: self.received(8, 9))
        at(5, lambda: self.received(10, 11))
        at(6, self.far)
        at(7, lambda: self.received(12, 13))


class Exchange:
    COPIES = 9

    def __init__(self, size, src, dst, via, sems, off):
        me, right, left, opp = ring(size)
        plan = [(src(opp), via.at[0], left), (src(swap_core(opp)), via.at[1], right)]
        plan += [(src(dev), dst(me), dev) for side in (right, left) for dev in (side, swap_core(side))]
        plan += [(src(swap_core(me)), dst(me), swap_core(me)), (via.at[0], dst(right), left), (via.at[1], dst(left), swap_core(right))]
        self.copy = lambda i: push(*plan[i][:2], sems[0].at[off + i], sems[1].at[off + i], plan[i][2])

    def start(self):
        for i in range(7):
            self.copy(i).start()

    def forward(self):
        for got, i in ((0, 7), (1, 8)):
            self.copy(got).wait_recv()
            self.copy(i).start()

    def close(self):
        for i in range(2, self.COPIES):
            self.copy(i).wait_recv()
        for i in range(self.COPIES):
            self.copy(i).wait_send()


def pair_rows(ref, c):
    return jnp.concatenate([ref[2 * c].astype(F32), ref[2 * c + 1].astype(F32)])


def pair_chunks(size, tok, body):
    pl.loop(0, size // 2)(lambda c: body(c, pl.ds(pl.multiple_of(c * 2 * tok, 16), 2 * tok)))


def cut(rows):
    half = rows // 2 // 16 * 16
    return pl.ds(0, half), pl.ds(half, rows - half)


def head(z, i, hd):
    return z[i * hd:(i + 1) * hd]


def norm_rows(z):
    centered = z - jnp.mean(z, axis=-1, keepdims=True)
    inv = lax.rsqrt(jnp.mean(centered * centered, axis=-1, keepdims=True) + LN_EPS)
    return centered * inv, inv


def norm_rows_pull(xhat, inv, dh, gain):
    dxh = dh * gain
    return inv * (dxh - jnp.mean(dxh, axis=-1, keepdims=True) - xhat * jnp.mean(dxh * xhat, axis=-1, keepdims=True))


def arrival(i, size):
    me = lax.axis_index('tp')
    partner = me + 1 - 2 * lax.rem(me, 2)
    hop = jnp.where(i < 2, 0, jnp.where(i >= 6, size // 2, jnp.where(lax.rem(i, 2) == 0, size - 2, 2)))
    base = jnp.where((i == 1) | (i == 4) | (i == 5) | (i == 7), partner, me)
    return lax.rem(base + hop, size)


def gelu_and_slope(u):
    c = math.sqrt(2.0 / math.pi)
    u2 = u * u
    t = jnp.tanh(c * (u + 0.044715 * (u2 * u)))
    half = 0.5 * (1.0 + t)
    slope = half + 0.5 * u * (1.0 - t * t) * (c * (1.0 + (3.0 * 0.044715) * u2))
    return u * half, slope


def front_kernel(heads, hd, size, x_ref, wq_ref, wk_ref, wv_ref, wo_ref, bq_ref, bv_ref, b1_ref,
                 g1_ref, c1_ref, g2_ref, c2_ref, bo_ref, b2_ref, w1_ref, w2_ref, do_ref,
                 qkv_ref, mix_ref, st_ref, h1_out, y_out, dm_out, sums_ref, w1t_out, xi_ref, wa_ref, doa_ref, h2a_ref,
                 h1_ref, y_ref, dm_ref, w1t_ref, wl_ref, w_all, w1_all, w2_all, x_all, via, acc_ref, dacc, own_do, d_img, xm_ref, h2_ref, loc_sem, out_sem, send_sem, recv_sem):
    hw = heads * hd
    scale = 1.0 / math.sqrt(hd)
    step = pl.program_id(0)
    k = step - size
    mlp = w2_ref.shape[0]
    me = lax.axis_index('tp')
    imgs, tok, width = x_ref.shape
    n = h1_ref.shape[0]
    g1, c1, g2, c2 = g1_ref[...], c1_ref[...], g2_ref[...], c2_ref[...]
    bo, b2 = (r[...].astype(F32).reshape(1, width) for r in (bo_ref, b2_ref))
    rows = wl_ref.shape[0]
    sems = send_sem, recv_sem
    images = pl.ds(0, imgs // 2), pl.ds(imgs // 2, imgs // 2)
    mine = lambda dev: pl.ds(pl.multiple_of(dev * tok, 8), tok)
    gw = Gather(size, lambda h: wl_ref.at[cut(rows)[h]], lambda d, h: w_all.at[d, cut(rows)[h]], sems, 0)
    gw1 = Gather(size, lambda h: w1_ref.at[cut(width)[h]], lambda d, h: w1_all.at[d, cut(width)[h]], sems, Gather.COPIES)
    gdo = Gather(size, lambda h: do_ref.at[images[h]], lambda d, h: doa_ref.at[images[h], mine(d)], sems, 2 * Gather.COPIES)
    gw2 = Gather(size, lambda h: w2_ref.at[cut(mlp)[h]], lambda d, h: w2_all.at[d, cut(mlp)[h]], sems, 3 * Gather.COPIES)
    gh2 = Gather(size, lambda h: h2_ref.at[cut(n)[h]], lambda d, h: h2a_ref.at[d, cut(n)[h]], sems, 4 * Gather.COPIES)
    ex = Exchange(size, lambda d: x_ref.at[d], lambda d: x_all.at[d], via, sems, 5 * Gather.COPIES)
    local = lambda src, dst, i: pltpu.make_async_copy(src, dst, loc_sem.at[i])
    in_x, in_do = local(x_ref.at[me], x_all.at[me], 0), local(do_ref, own_do, 1)
    out_w, out_h2 = local(wl_ref, wa_ref.at[me], 2), local(h2_ref, h2a_ref.at[me], 3)
    in_img = local(doa_ref.at[me], d_img, 6)
    out_h1, out_w1t, out_y, out_dm = local(h1_ref, h1_out, 7), local(w1t_ref, w1t_out, 8), local(y_ref, y_out, 9), local(dm_ref, dm_out, 10)
    out_x, out_do = local(x_all, xi_ref, 4), local(own_do, doa_ref.at[:, mine(me)], 5)

    def out_block(i):
        dev = arrival(i, size)
        return pltpu.make_async_copy(w_all.at[dev], wa_ref.at[dev], out_sem.at[i])

    @pl.when(step == 0)
    def _():
        in_x.start()
        in_do.start()
        greet_all(size)
        ex.start()
        for i, part in enumerate((wq_ref, wk_ref, wv_ref, wo_ref)):
            wl_ref[i * hw:(i + 1) * hw] = part[...]
        zeros = jnp.zeros((1, hw), F32)
        pieces = [r[h:h + 1].astype(F32) for r in (bq_ref, bv_ref) for h in range(heads)]
        line = jnp.concatenate(pieces[:heads] + [zeros] + pieces[heads:] + [b1_ref[...].astype(F32).reshape(1, mlp)]
                               + [zeros] * ((width - 3 * hw - mlp) // hw), axis=1)
        wl_ref[4 * hw:] = jnp.where(lax.broadcasted_iota(jnp.int32, (BIAS_ROWS, width), 0) == 0, line, 0.0).astype(BF16)
        ex.forward()
        gw.start()
        out_w.start()
        w_all[me] = wl_ref[...]
        in_x.wait()
        ex.close()
        out_x.start()

        def body(c, rows):
            xhat, _ = norm_rows(pair_rows(x_all, c))
            h1_ref[rows] = (xhat * g1 + c1).astype(BF16)

        pair_chunks(size, tok, body)
        in_do.wait()
        out_do.start()

    gw.follow(step, gw.forward, gdo.start)

    @pl.when((step > 0) & (k < 0))
    def _():
        out_block(step).start()

    @pl.when(k < 0)
    def _():
        w = w_all.at[arrival(step, size)]
        bias = mm(w[4 * hw:, :3 * hw], jnp.ones((BIAS_ROWS, n), BF16), TN)
        qkv = (mm(w[:3 * hw], h1_ref[...], NT) + bias).astype(BF16)
        qkv_ref[0] = qkv
        for h in range(heads):
            q, key, v = (head(qkv, i * heads + h, hd) for i in range(3))
            s = mm(key, q, TN) * scale
            top = jnp.max(s, axis=0, keepdims=True)
            e = jnp.exp(s - top)
            inv = 1.0 / jnp.sum(e, axis=0, keepdims=True)
            st_ref[0, h:h + 1] = top
            st_ref[0, heads + h:heads + h + 1] = inv
            mix_ref[0, h * hd:(h + 1) * hd] = mm(v, (e * inv).astype(BF16), NN).astype(BF16)
        out = mm(mix_ref[0], w[3 * hw:4 * hw], TN)

        @pl.when(step == 0)
        def _():
            acc_ref[...] = out

        @pl.when(step > 0)
        def _():
            acc_ref[...] += out

    @pl.when(k == -1)
    def _():
        gdo.forward()
        gw1.start()

        def body(c, rows):
            mid = (pair_rows(x_all, c) + acc_ref[rows] + bo).astype(BF16)
            xm_ref[rows] = mid
            xhat, _ = norm_rows(mid.astype(F32))
            h2_ref[rows] = (xhat * g2 + c2).astype(BF16)

        pair_chunks(size, tok, body)

    @pl.when(k == 0)
    def _():
        out_h2.start()
        w1_all[me] = w1_ref[...]
        w2_all[me] = w2_ref[...]
        w1t_ref[...] = w1_ref[...].T
        gdo.near()
        gdo.far()
        gw1.forward()
        gw2.start()
        gdo.received(*range(6, Gather.COPIES))
        out_do.wait()
        in_img.start()
        in_img.wait()

    gw1.follow(k, out_h1.start, out_w1t.start)
    gw2.follow(k, gw2.forward, gh2.start)

    @pl.when(k >= 0)
    def _():
        dev = arrival(k, size)
        w1, w2 = w1_all[dev], w2_all[dev]
        b1 = w_all[dev, 4 * hw:4 * hw + 1, 3 * hw:3 * hw + mlp].astype(F32)
        u = (mm(h2_ref[...], w1, NN) + b1).astype(BF16).astype(F32)
        dg = mm(d_img[...], w2, NT).astype(BF16).astype(F32)
        g, slope = gelu_and_slope(u)
        ypart = mm(g.astype(BF16), w2, NN)
        dpart = mm((dg * slope).astype(BF16), w1, NT)

        @pl.when(k == 0)
        def _():
            acc_ref[...] = ypart
            dacc[...] = dpart

        @pl.when(k > 0)
        def _():
            acc_ref[...] += ypart
            dacc[...] += dpart

    @pl.when(k == size - 1)
    def _():
        sums_ref[...] = jnp.zeros_like(sums_ref)

        def body(c, part):
            mid = xm_ref[part].astype(F32)
            y_ref[part] = (mid + acc_ref[part] + b2).astype(BF16)
            xhat, inv = norm_rows(mid)
            dh = dacc[part].astype(BF16).astype(F32)
            do = d_img[part].astype(F32)
            dm = (do + norm_rows_pull(xhat, inv, dh, g2)).astype(BF16)
            dm_ref[part] = dm
            for i, v in enumerate((dh * xhat, dh, dm.astype(F32), do)):
                sums_ref[2 + i:3 + i] += jnp.sum(v, axis=0, keepdims=True)

        gh2.forward()
        pair_chunks(size, tok, body)
        gh2.near()
        out_y.start()
        out_dm.start()
        gh2.far()
        gh2.received(*range(6, Gather.COPIES))
        for g in (gw, gw1, gdo, gw2, gh2):
            g.sent()
        for c in (out_x, out_w, out_h2, out_h1, out_w1t, out_y, out_dm):
            c.wait()
        for i in range(1, size):
            out_block(i).wait()


def whole(*shape):
    return pl.BlockSpec(shape, lambda i: (0,) * len(shape), pipeline_mode=pl.Buffered(1))


def block(index, *shape):
    return pl.BlockSpec((1,) + shape, lambda i: (index(i),) + (0,) * len(shape))


def dma(k):
    return pltpu.SemaphoreType.DMA((k,))


def kernel_params(collective_id):
    return pltpu.CompilerParams(dimension_semantics=("arbitrary",), vmem_limit_bytes=67_043_328,
                                collective_id=collective_id, has_side_effects=True)


ANY = pl.BlockSpec(memory_space=pl.ANY)


def front(x, weights, biases, gains, sums_bias, w_1, w_2, d_out, heads, hd):
    imgs, tok, width = x.shape
    size = imgs
    n = size * tok
    hw = heads * hd
    mlp = w_2.shape[0]
    rows = 4 * hw + BIAS_ROWS
    order = lambda i: arrival(jnp.minimum(i, size - 1), size)
    bf = lambda *shape: jax.ShapeDtypeStruct(shape, BF16)
    buf = lambda *shape: pltpu.VMEM(shape, BF16)
    copies = 5 * Gather.COPIES + Exchange.COPIES
    return pl.pallas_call(
        functools.partial(front_kernel, heads, hd, size),
        grid=(2 * size,),
        in_specs=[ANY] + [whole(*z.shape) for z in weights + biases + gains + sums_bias] + [ whole(width, mlp), whole(mlp, width), ANY],
        out_specs=[block(order, 3 * hw, n), block(order, hw, n), block(order, 2 * heads, n), ANY, ANY, ANY, whole(8, width)]
                  + [ANY] * 5,
        out_shape=[bf(size, 3 * hw, n), bf(size, hw, n), jax.ShapeDtypeStruct((size, 2 * heads, n), F32), bf(n, width), bf(n, width),
                   bf(n, width), jax.ShapeDtypeStruct((8, width), F32), bf(mlp, width),
                   bf(size, tok, width), bf(size, rows, width), bf(imgs, n, width), bf(size, n, width)],
        scratch_shapes=[buf(n, width), buf(n, width), buf(n, width), buf(mlp, width), buf(rows, width), buf(size, rows, width), buf(size, width, mlp), buf(size, mlp, width), buf(size, tok, width), buf(2, tok, width),
                        pltpu.VMEM((n, width), F32), pltpu.VMEM((n, width), F32), buf(*d_out.shape), buf(n, width), buf(n, width),
                        buf(n, width), dma(11), dma(size), dma(copies), dma(copies)],
        compiler_params=kernel_params(1),
        name="front",
    )(x, *weights, *biases, *gains, *sums_bias, w_1, w_2, d_out)


def block_of_step(j, size):
    me = lax.axis_index('tp')
    chips = size // 2
    off = jnp.where(j < 2, 2, jnp.where(j < 4, 1, jnp.where(j < 6, 3, 0)))
    chip = lax.rem(lax.div(me, 2) + off, chips)
    core = lax.rem(me, 2)
    side = jnp.where(lax.rem(j, 2) == 0, 1 - core, core)
    return 2 * chip + side


def back_kernel(heads, hd, size, h_ref, dm_ref, w_ref, qkv_ref, mix_ref, st_ref, h2_ref, do_ref, w1_in, w2_in, b_ref,
                x3_in, dm3_in, y3_ref, gain_ref, vin_ref,
                g_out, gw1_out, gw2_out, gb1_ref, gx_ref, vec_ref, yo_ref,
                w1_ref, w2_ref, x3_ref, dm3_ref, g_ref, gw1_ref, gw2_ref,
                dqkv_ref, dh_ref, gx_own, v_own, v_all, via_y, via_g,
                outs, pair_in, opp_l, opp_r, near_l, near_r, acc, loc_sem, send_sem, recv_sem):
    hw = heads * hd
    half = 2 * hw
    scale = 1.0 / math.sqrt(hd)
    j = pl.program_id(0)
    m = j - size
    me, right, left, _ = ring(size)
    partner = swap_core(me)
    n, width = h_ref.shape
    rows = outs.shape[1]
    tok = x3_ref.shape[1]
    mlp = w2_ref.shape[0]
    sems = send_sem, recv_sem
    own = 2
    base = 0
    ex_y = Exchange(size, lambda d: y3_ref.at[d], lambda d: yo_ref.at[d], via_y, sems, base)
    base += Exchange.COPIES
    ex_g = Exchange(size, lambda d: gx_own.at[d], lambda d: gx_ref.at[d], via_g, sems, base)
    base += Exchange.COPIES
    local = lambda src, dst, i: pltpu.make_async_copy(src, dst, loc_sem.at[i])
    y_local, gx_local = local(y3_ref.at[me], yo_ref.at[me], 1), local(gx_own.at[me], gx_ref.at[me], 2)
    late = [local(src, dst, 3 + i) for i, (src, dst) in enumerate(((x3_in, x3_ref), (dm3_in, dm3_ref), (w1_in, w1_ref), (w2_in, w2_ref)))]
    outward = [local(src, dst, 7 + i) for i, (src, dst) in enumerate(((gw1_ref, gw1_out), (gw2_ref, gw2_out), (g_ref, g_out)))]

    def numbered(src, dst, i, dev):
        return push(src, dst, send_sem.at[base + i], recv_sem.at[base + i], dev)

    def pair_copy(t):
        return numbered(outs.at[t % own], pair_in.at[t % own], t, partner)

    pairs = size // 2
    lo, hi = pl.ds(0, half), pl.ds(half, rows - half)
    one, two = own + 1, own + 2
    opp_right = lambda: numbered(outs.at[own, lo], opp_l, pairs, right)
    opp_left = lambda: numbered(outs.at[own, hi], opp_r, pairs + 1, left)
    right_hi = lambda: numbered(outs.at[one, hi], near_l.at[hi], pairs + 2, right)
    right_lo = lambda: numbered(outs.at[one, lo], near_l.at[lo], pairs + 3, right)
    left_lo = lambda: numbered(outs.at[two, lo], near_r.at[lo], pairs + 4, left)
    left_hi = lambda: numbered(outs.at[two, hi], near_r.at[hi], pairs + 5, left)

    def v_copy(dev, slot):
        return push(v_own, v_all.at[slot], send_sem.at[base + 2 * size + dev], recv_sem.at[base + 2 * size + slot], dev)

    @pl.when(j == 0)
    def _():
        greet_all(size)
        ex_y.start()
        y_local.start()
        for c in late:
            c.start()

    @pl.when(j == 1)
    def _():
        ex_y.forward()

    @pl.when(j < size)
    def _():
        d_mix = mm(dm_ref[...], w_ref[0, 3 * hw:4 * hw], NT).astype(BF16).T
        qkv = qkv_ref[0]
        for h in range(heads):
            q, k, v = (head(qkv, i * heads + h, hd) for i in range(3))
            da = head(d_mix, h, hd)
            s = mm(k, q, TN) * scale
            p = jnp.exp(s - st_ref[0, h:h + 1]) * st_ref[0, heads + h:heads + h + 1]
            dp = mm(v, da, TN).astype(BF16).astype(F32)
            ds = (p * (dp - jnp.sum(p * dp, axis=0, keepdims=True)) * scale).astype(BF16)
            dk = mm(ds, q, NT).astype(BF16).T
            dv = mm(p.astype(BF16), da, NT).astype(BF16).T
            for i, z in enumerate((mm(k, ds, NN).astype(BF16), dk, dv)):
                at = i * hw + h * hd
                dqkv_ref[at:at + hd] = z
        dqkv = dqkv_ref[...]
        part = mm(dqkv, w_ref[0, :3 * hw], TN)

        @pl.when(j == 0)
        def _():
            dh_ref[...] = part

        @pl.when(j > 0)
        def _():
            dh_ref[...] += part

        for t in range(own, pairs):
            @pl.when(j == 2 * t)
            def _():
                pair_copy(t - own).wait_send()

        @pl.when(j == size - 1)
        def _():
            opp_right().wait_send()
            opp_left().wait_send()

        turn = lax.div(j, 2)
        out = outs.at[jnp.where(lax.rem(j, 2) == 0, lax.rem(turn, own), own + lax.rem(turn, pairs - 1))]
        out[:3 * hw] = mm(dqkv, h_ref[...], NN)
        out[3 * hw:4 * hw] = mm(mix_ref[0], dm_ref[...], NN)
        sums = mm(jnp.ones((BIAS_ROWS, n), BF16), dqkv, NT)
        out[4 * hw:] = jnp.concatenate([sums, jnp.zeros((BIAS_ROWS, width - 3 * hw), F32)], axis=1)

        for t in range(pairs):
            @pl.when(j == 2 * t)
            def _():
                pair_copy(t).start()

            @pl.when(j == 2 * t + 1)
            def _():
                pair_copy(t).wait_recv()
                outs[own + t % (pairs - 1)] += pair_in[t % own]

        @pl.when(j == 1)
        def _():
            opp_right().start()
            opp_left().start()

        @pl.when(j == 3)
        def _():
            right_hi().start()

        @pl.when(j == 5)
        def _():
            left_lo().start()

        @pl.when(j == size - 1)
        def _():
            opp_right().wait_recv()
            outs[one, lo] += opp_l[...]
            right_lo().start()
            opp_left().wait_recv()
            outs[two, hi] += opp_r[...]
            left_hi().start()

    @pl.when(m == 0)
    def _():
        v_own[...] = vin_ref[...]
        for c in late:
            c.wait()

        @pl.loop(0, size)
        def _(dev):
            dh = dh_ref[pl.ds(pl.multiple_of(dev * tok, 8), tok)].astype(BF16).astype(F32)
            xhat, inv = norm_rows(x3_ref[dev].astype(F32))
            gx_own[dev] = (dm3_ref[dev].astype(F32) + norm_rows_pull(xhat, inv, dh, gain_ref[...])).astype(BF16)
            v_own[0:1] += jnp.sum(dh * xhat, axis=0, keepdims=True)
            v_own[1:2] += jnp.sum(dh, axis=0, keepdims=True)

        ex_g.start()
        for r in range(1, size):
            v_copy(lax.rem(me + r, size), me).start()
        gx_local.start()
        v_all[me] = v_own[...]

    @pl.when(m == size - 1)
    def _():
        ex_g.forward()

    @pl.when(m >= 0)
    def _():
        h2 = h2_ref[0]
        do = do_ref[0]
        one_row = (lax.broadcasted_iota(jnp.int32, (BIAS_ROWS, n), 0) == 0).astype(F32).astype(BF16)
        b1 = mm(b_ref[0, :, 3 * hw:3 * hw + mlp], one_row, TN)
        u = (mm(w1_ref[...], h2, NT) + b1).astype(BF16).astype(F32)
        dg = mm(w2_ref[...], do, NT).astype(BF16).astype(F32)
        g, slope = gelu_and_slope(u)
        du = (dg * slope).astype(BF16)
        g1 = mm(du, h2, NN)
        g2 = mm(g.astype(BF16), do, NN)
        gb = mm(jnp.ones((8, n), BF16), du, NT)

        @pl.when(m == 0)
        def _():
            acc[:mlp] = g1
            acc[mlp:] = g2
            gb1_ref[...] = gb

        @pl.when(m > 0)
        def _():
            acc[:mlp] += g1
            acc[mlp:] += g2
            gb1_ref[...] += gb

    @pl.when(m == size - 1)
    def _():
        gw1_ref[...] = acc[:mlp].astype(BF16)
        gw2_ref[...] = acc[mlp:].astype(BF16)
        ring_copies = (right_hi(), right_lo(), left_lo(), left_hi())
        for c in ring_copies:
            c.wait_recv()
        outward[0].start()
        outward[1].start()
        g_ref[...] = (outs[own] + near_l[...] + near_r[...]).astype(BF16)
        for c in ring_copies + (pair_copy(pairs - 2), pair_copy(pairs - 1)):
            c.wait_send()
        for r in range(1, size):
            dev = lax.rem(me + r, size)
            v_copy(dev, dev).wait()
        total = v_all[0]
        for i in range(1, size):
            total += v_all[i]
        vec_ref[...] = total
        outward[2].start()
        ex_y.close()
        ex_g.close()
        gx_local.wait()
        y_local.wait()
        for c in outward:
            c.wait()


def back(h_one, d_mid, wcat, qkv, mix, stats, h2_all, d_out_all, w1t, w_2, x3, y_img, gain, sums, heads, hd):
    size, rows, width = wcat.shape
    n = h_one.shape[0]
    mlp = w_2.shape[0]
    hw = heads * hd
    first = lambda i: block_of_step(jnp.minimum(i, size - 1), size)
    second = lambda i: jnp.maximum(i - size, 0)
    buf = lambda *shape: pltpu.VMEM(shape, F32)
    half_buf = lambda *shape: pltpu.VMEM(shape, BF16)
    bf = lambda *shape: jax.ShapeDtypeStruct(shape, BF16)
    copies = 2 * Exchange.COPIES + 3 * size
    half = 2 * hw
    tokens = x3.shape[1:]
    act3 = whole(*x3.shape)
    return pl.pallas_call(
        functools.partial(back_kernel, heads, hd, size),
        grid=(2 * size,),
        in_specs=[whole(n, width), whole(n, width), block(first, rows, width), block(first, 3 * hw, n), block(first, hw, n),
                  block(first, 2 * heads, n), block(second, n, width), block(second, n, width), ANY, ANY,
                  pl.BlockSpec((1, BIAS_ROWS, width), lambda i: (lax.axis_index('tp'), rows // BIAS_ROWS - 1, 0)),
                  ANY, ANY, act3, whole(1, width), whole(*sums.shape)],
        out_specs=[ANY, ANY, ANY, whole(8, mlp), ANY, whole(*sums.shape), ANY],
        out_shape=[bf(rows, width), bf(mlp, width), bf(mlp, width), jax.ShapeDtypeStruct((8, mlp), F32), bf(*x3.shape),
                   jax.ShapeDtypeStruct(sums.shape, F32), bf(*x3.shape)],
        scratch_shapes=[half_buf(mlp, width), half_buf(mlp, width), half_buf(*x3.shape), half_buf(*x3.shape), half_buf(rows, width),
                        half_buf(mlp, width), half_buf(mlp, width), half_buf(3 * hw, n), buf(n, width), half_buf(*x3.shape), buf(*sums.shape), buf(size, *sums.shape),
                        half_buf(2, *tokens), half_buf(2, *tokens), buf(size // 2 + 1, rows, width), buf(2, rows, width),
                        buf(half, width), buf(rows - half, width), buf(rows, width), buf(rows, width), buf(2 * mlp, width),
                        dma(10), dma(copies), dma(copies)],
        compiler_params=kernel_params(2),
        name="back",
    )(h_one, d_mid, wcat, qkv, mix, stats, h2_all, d_out_all, w1t, w_2, wcat, x3, d_mid.reshape(x3.shape), y_img.reshape(x3.shape),
      gain, sums)


def finish_kernel(heads, hd, g_ref, gw1_ref, gw2_ref, gb1_ref, gx_ref, y_ref, vec_ref,
                  gq, gk, gv, go, bq, bv, w1_out, b1_out, w2_out, x_out, y_out, *vec_outs):
    hw = heads * hd
    for i, out in enumerate((gq, gk, gv, go)):
        out[...] = g_ref[i * hw:(i + 1) * hw]
    sums = g_ref[4 * hw:].astype(F32)[:1]
    for i, out in ((0, bq), (2, bv)):
        for h in range(heads):
            at = i * hw + h * hd
            out[h:h + 1] = sums[:, at:at + hd].astype(BF16)
    w1_out[...] = gw1_ref[...].T
    b1_out[...] = gb1_ref[0].astype(BF16)
    w2_out[...] = gw2_ref[...]
    x_out[...] = gx_ref[...]
    y_out[...] = y_ref[...]
    for i, out in enumerate(vec_outs):
        out[...] = vec_ref[i].astype(out.dtype)


def finish(g, gw1, gw2, gb1, gx, y, vec, heads, hd):
    width = g.shape[1]
    mlp = gw2.shape[0]
    hw = heads * hd
    bf = lambda *shape: jax.ShapeDtypeStruct(shape, BF16)
    f32_row = jax.ShapeDtypeStruct((width,), F32)
    vm = pl.BlockSpec(memory_space=pltpu.VMEM)
    outs = [bf(hw, width)] * 4 + [bf(heads, hd)] * 2 + [bf(width, mlp), bf(mlp), bf(mlp, width), bf(*gx.shape), bf(*y.shape)]
    outs += [f32_row] * 4 + [bf(width)] * 2
    return pl.pallas_call(
        functools.partial(finish_kernel, heads, hd),
        in_specs=[vm] * 7,
        out_specs=[vm] * len(outs),
        out_shape=outs,
        compiler_params=pltpu.CompilerParams(vmem_limit_bytes=67_043_328),
        name="finish",
    )(g, gw1, gw2, gb1, gx, y, vec)


def solution(mesh):
    act_spec = P('dp', 'tp', None)
    replicated = P()
    head_w = P(None, 'tp', None)
    head_b = P('tp', None)
    grad_head_w = P('dp', 'tp', None)
    grad_head_b = P(('dp', 'tp'), None)
    grad_vec = P('dp')
    in_specs = (act_spec, act_spec, replicated, replicated, head_w, head_b, head_w, head_w, head_b,
                P('tp', None, None), replicated, replicated, replicated, P(None, 'tp'), P('tp'), P('tp', None), replicated)
    out_specs = (act_spec, act_spec, grad_vec, grad_vec, grad_head_w, grad_head_b, grad_head_w, grad_head_w, grad_head_b,
                 P(('dp', 'tp'), None, None), grad_vec, grad_vec, grad_vec, P('dp', 'tp'), P(('dp', 'tp')),
                 P(('dp', 'tp'), None), grad_vec)

    def layer_step(x, d_out, ln1_gain, ln1_bias, w_q, b_q, w_k, w_v, b_v, w_o, b_o, ln2_gain, ln2_bias, w_1, b_1, w_2, b_2):
        width = x.shape[-1]
        heads_loc, hd = w_q.shape[1:]
        hw = heads_loc * hd
        flat = lambda w: w.transpose(1, 2, 0).reshape(hw, width)
        qkv, mixed, stats, h_one, y_img, d_mid, sums, w1t, x_img, wcat, d_out_all, h2_all = front(
            x, (flat(w_q), flat(w_k), flat(w_v), w_o.reshape(hw, width)), (b_q, b_v, b_1),
            (ln1_gain[None], ln1_bias[None], ln2_gain[None], ln2_bias[None]), (b_o, b_2), w_1, w_2, d_out, heads_loc, hd)
        g_all, gw1, gw2, gb1, gx, vec, y_tok = back(
            h_one, d_mid, wcat, qkv, mixed, stats, h2_all, d_out_all, w1t, w_2, x_img, y_img, ln1_gain[None], sums, heads_loc, hd)
        (gq, gk, gv, go, grad_b_q, grad_b_v, grad_w_1, grad_b_1, grad_w_2, grad_x, y_out, g_ln1_gain, g_ln1_bias, g_ln2_gain, g_ln2_bias,
         grad_b_o, grad_b_2) = finish(g_all, gw1, gw2, gb1, gx, y_tok, vec, heads_loc, hd)
        gq, gk, gv = (z.reshape(heads_loc, hd, width).transpose(2, 0, 1) for z in (gq, gk, gv))
        grad_w_o = go.reshape(w_o.shape)
        return (y_out, grad_x, g_ln1_gain, g_ln1_bias, gq, grad_b_q, gk, gv, grad_b_v, grad_w_o,
                grad_b_o, g_ln2_gain, g_ln2_bias, grad_w_1, grad_b_1, grad_w_2, grad_b_2)

    return jax.shard_map(layer_step, mesh=mesh, in_specs=in_specs, out_specs=out_specs, check_vma=False)
```
